8 devices in a mesh: vp: 8 (over z, y, x, core).
Axes of the slice: x: 2, y: 2, z: 1, core: 2. Of those that a mesh axis runs over, the one named last changes fastest.
Arguments:
- residual: bfloat16 [1024, 1024], replicated
- labels: int32 [1024], replicated
- loss_mask: float32 [1024], replicated
- norm_gain: float32 [1024], replicated
- embed_table: bfloat16 [49408, 1024], P('vp')
Outputs:
- output 1: float32 [], replicated
- output 2: float32 [1024, 1024], P('vp')
- output 3: float32 [49408, 1024], P('vp')
- output 4: float32 [1024], replicated
All inputs are finite; a program needn't handle non-finite values.
Results may differ from the reference program's by a relative error of at most 0.001.
Values sent between devices are 32-bit elements.
A program may use at most 1 GiB of HBM per device.

```python
import jax
import jax.numpy as jnp
from jax import lax

TOKENS = 1024
DIM = 1024
VOCAB_REAL = 49155
VOCAB_PAD = 49408

LOGIT_SCALE = 6.0
NORM_EPS = 1e-6


def draw_labels(label_key):
    k_pick, k_wide, k_low = jax.random.split(label_key, 3)
    pick_wide = jax.random.randint(k_pick, (TOKENS,), 0, 2)
    wide_ids = jax.random.randint(k_wide, (TOKENS,), 0, VOCAB_REAL)
    low_ids = jax.random.randint(k_low, (TOKENS,), 0, VOCAB_REAL // 16)
    label_ids = jnp.where(pick_wide == 0, wide_ids, low_ids).astype(jnp.int32)
    return label_ids.at[0].set(0).at[1].set(VOCAB_REAL - 1)


def draw_mask(mask_key):
    keep_draw = jax.random.randint(mask_key, (TOKENS,), 0, 5)
    mask_vals = (keep_draw > 0).astype(jnp.float32)
    return mask_vals.at[0].set(1.0)


def setup_inputs(seed: int = 0) -> dict:
    base_key = jax.random.key(seed)
    k_table, k_noise, k_peak, k_gain, k_label, k_mask = jax.random.split(base_key, 6)
    emb_std = LOGIT_SCALE * DIM ** -0.5
    table_f32 = jax.random.normal(k_table, (VOCAB_PAD, DIM), jnp.float32) * emb_std
    peak_ids = jax.random.randint(k_peak, (TOKENS, 4), 0, VOCAB_REAL)
    peak_sum = jnp.zeros((TOKENS, DIM), jnp.float32)
    for peak in range(4):
        peak_sum = peak_sum + table_f32[peak_ids[:, peak]] / emb_std
    peak_weight = 14.0 * DIM ** -0.5
    noise = jax.random.normal(k_noise, (TOKENS, DIM), jnp.float32)
    residual = (noise + peak_weight * peak_sum).astype(jnp.bfloat16)
    norm_gain = 1.0 + 0.3 * jax.random.normal(k_gain, (DIM,), jnp.float32)
    return {
        'residual': residual,
        'labels': draw_labels(k_label),
        'loss_mask': draw_mask(k_mask),
        'norm_gain': norm_gain,
        'embed_table': table_f32.astype(jnp.bfloat16),
    }


def reference(residual, labels, loss_mask, norm_gain, embed_table):
    x_f32 = residual.astype(jnp.float32)
    inv_rms = lax.rsqrt(jnp.mean(x_f32 * x_f32, axis=-1, keepdims=True) + NORM_EPS)
    x_hat = x_f32 * inv_rms
    hidden = (x_hat * norm_gain).astype(jnp.bfloat16)
    mask_total = jnp.sum(loss_mask)
    tok_weight = loss_mask / mask_total
    col_ids = jnp.arange(VOCAB_PAD)[None, :]
    row_block = min(TOKENS, 256)
    n_blocks = TOKENS // row_block

    def block_step(grad_table, block_in):
        h_blk, lab_blk, w_blk = block_in
        logits = jnp.dot(h_blk, embed_table.T, preferred_element_type=jnp.float32) / LOGIT_SCALE
        logits = jnp.where(col_ids < VOCAB_REAL, logits, -jnp.inf)
        row_max = jnp.max(logits, axis=-1, keepdims=True)
        shifted = jnp.exp(logits - row_max)
        sum_exp = jnp.sum(shifted, axis=-1, keepdims=True)
        is_label = col_ids == lab_blk[:, None]
        target = jnp.sum(jnp.where(is_label, logits, 0.0), axis=-1)
        tok_loss = row_max[:, 0] + jnp.log(sum_exp[:, 0]) - target
        row_prob = shifted / sum_exp
        d_logits = (jnp.where(is_label, row_prob - 1.0, row_prob) * w_blk[:, None]).astype(jnp.bfloat16)
        d_hidden = jnp.dot(d_logits, embed_table, preferred_element_type=jnp.float32) / LOGIT_SCALE
        grad_table = grad_table + jnp.dot(d_logits.T, h_blk, preferred_element_type=jnp.float32) / LOGIT_SCALE
        return grad_table, (tok_loss, d_hidden)

    blocks = (hidden.reshape(n_blocks, row_block, DIM), labels.reshape(n_blocks, row_block), tok_weight.reshape(n_blocks, row_block))
    d_embed, (tok_loss, d_hidden) = lax.scan(block_step, jnp.zeros((VOCAB_PAD, DIM), jnp.float32), blocks)
    tok_loss = tok_loss.reshape(TOKENS)
    d_hidden = d_hidden.reshape(TOKENS, DIM)
    mean_loss = jnp.sum(loss_mask * tok_loss) / mask_total
    d_gain = jnp.sum(d_hidden * x_hat, axis=0)
    d_xhat = d_hidden * norm_gain
    d_residual = inv_rms * (d_xhat - x_hat * jnp.mean(d_xhat * x_hat, axis=-1, keepdims=True))
    return (mean_loss, d_residual, d_embed, d_gain)
```

```python
import functools

import jax
import jax.numpy as jnp
from jax import lax
from jax.experimental import pallas as pl
from jax.experimental.pallas import tpu as pltpu
from jax.sharding import PartitionSpec as P

VOCAB_REAL = 49155
LOGIT_SCALE = 6.0
NORM_EPS = 1e-6
LOG2E = 1.4426950408889634
F32 = jnp.float32
BF16 = jnp.bfloat16
MESH = pl.DeviceIdType.MESH

N_DEV = 8
TOKENS = 1024
DIM = 1024
ROWS = 6176
CHUNKS = 4
CTOK = 256
PIECE = 32
HALF = DIM // 2
L_TILE = 256
K_TILE = 1024
DZ_BLOCK = 16
MASK_FROM = VOCAB_REAL - (N_DEV - 1) * ROWS
EXP_SCALE = LOG2E / LOGIT_SCALE


def split_rows(step):
    cuts = [[i * step, step] for i in range(ROWS // step)]
    cuts[-1][1] = ROWS - cuts[-1][0]
    return [tuple(c) for c in cuts]


TILES = split_rows(L_TILE)
KTILES = split_rows(K_TILE)
N_TILES = len(TILES)


def fold8(v):
    return jnp.sum(v.reshape(v.shape[0] // 8, 8, v.shape[1]), axis=0)


def interleave(main, side, ratio):
    main_done = side_done = False
    while not (main_done and side_done):
        if not main_done:
            main_done = next(main, 0) == 0
        for _ in range(ratio):
            if not side_done:
                side_done = next(side, 0) == 0


def main_kernel(x_hbm, y_in, m_in, g_in, e_hbm,
                dz_hbm, h_hbm, dx_out, dg_out, loss_out,
                emb, xv, hs, ht, rcol, ebuf, dzb, acc, ub0, ub1, yrow, mrow,
                tmax, tsum, crow, tgt, stx, srx, lossv, dgv, dgrx, ra, rb, rc,
                in_sem, h_sem, dz_sem, st_send, st_recv, rs_send, rs_recv, dg_send, dg_recv):
    me = lax.axis_index("vp")
    core = lax.rem(me, 2)
    xc = lax.rem(me // 2, 2)
    yc = me // 4
    peer_core = me + 1 - 2 * core
    peer_x = me + 2 - 4 * xc
    peer_y = me + 4 - 8 * yc

    mid_row = TILES[N_TILES // 2][0]
    e_copies = [
        pltpu.make_async_copy(e_hbm.at[pl.ds(0, mid_row)], emb.at[pl.ds(0, mid_row)], in_sem.at[0]),
        pltpu.make_async_copy(e_hbm.at[pl.ds(mid_row, ROWS - mid_row)], emb.at[pl.ds(mid_row, ROWS - mid_row)], in_sem.at[1]),
    ]
    x_copies = [pltpu.make_async_copy(x_hbm.at[:, c], xv.at[c], in_sem.at[2 + c]) for c in range(CHUNKS)]
    x_copies[0].start()
    e_copies[0].start()
    e_copies[1].start()
    for c in range(1, CHUNKS):
        x_copies[c].start()

    barrier = pltpu.get_barrier_semaphore()
    for k in range(1, N_DEV):
        pl.semaphore_signal(barrier, inc=1, device_id=(lax.rem(me + k, N_DEV),), device_id_type=MESH)

    lane = lax.broadcasted_iota(jnp.int32, (1, 128), 1) // PIECE
    base = me * ROWS
    for c in range(CHUNKS):
        for half in range(2):
            yh = jnp.zeros((1, 128), jnp.int32)
            mh = jnp.zeros((1, 128), F32)
            for i in range(4):
                row = half * 4 + i
                shift = (PIECE * (i - c)) % 128
                yr, mr = y_in[row:row + 1, :], m_in[row:row + 1, :]
                if shift:
                    yr, mr = pltpu.roll(yr, shift, 1), pltpu.roll(mr, shift, 1)
                yh = jnp.where(lane == i, yr, yh)
                mh = jnp.where(lane == i, mr, mh)
            yrow[c, :, half * 128:half * 128 + 128] = yh - base
            mrow[c, :, half * 128:half * 128 + 128] = mh
    mask_total = jnp.sum(jnp.sum(m_in[...], axis=0, keepdims=True), axis=1, keepdims=True)
    lossv[...] = jnp.zeros_like(lossv)
    dgv[...] = jnp.zeros_like(dgv)
    limit = VOCAB_REAL - base

    def norm_chunk(c):
        g = g_in[...]
        for r in range(CTOK // PIECE):
            xf = xv[c, r].astype(F32)
            inv = lax.rsqrt(jnp.mean(xf * xf, axis=1, keepdims=True) + NORM_EPS)
            rcol[c, r] = jnp.broadcast_to(inv, (PIECE, 128))
            hs[c, r * PIECE:(r + 1) * PIECE, :] = (xf * inv * g).astype(BF16)
        ht[c] = hs[c].T

    def logits(c, lo, hi, tg):
        slot = lax.rem(c, 2)
        iota = lax.broadcasted_iota(jnp.int32, (8, CTOK), 0)
        y = yrow[c]
        eb = ebuf.at[slot]
        ubs = (ub0, ub1)
        state = [tg]

        def mm(i):
            s, n = TILES[i]
            ubs[i % 2][0:n, :] = jnp.dot(emb[s:s + n, :], ht[c], preferred_element_type=F32)
            yield 1

        def post(i):
            s, n = TILES[i]
            u_ref = ubs[i % 2]
            m8 = jnp.full((8, CTOK), -jnp.inf, F32)
            for r in range(0, n, 8):
                u = u_ref[r:r + 8, :]
                if s + r + 8 > MASK_FROM:
                    u = jnp.where(iota < limit - (s + r), u, -jnp.inf)
                    u_ref[r:r + 8, :] = u
                m8 = jnp.maximum(m8, u)
            m = jnp.max(m8, axis=0, keepdims=True)
            s8 = jnp.zeros((8, CTOK), F32)
            for r in range(0, n, 8):
                u = u_ref[r:r + 8, :]
                e = jnp.exp2((u - m) * EXP_SCALE)
                eb[s + r:s + r + 8, :] = e
                s8 = s8 + e
                state[0] = state[0] + jnp.where(iota == (y - (s + r)), u, 0.0)
                if r % 64 == 56:
                    yield 1
            tmax[slot, i:i + 1, :] = m
            tsum[slot, i:i + 1, :] = jnp.sum(s8, axis=0, keepdims=True)
            yield 1

        for _ in mm(lo):
            pass
        for i in range(lo + 1, hi):
            interleave(mm(i), post(i - 1), 6)
        for _ in post(hi - 1):
            pass
        return state[0]

    def stat_copy(c, k):
        return pltpu.make_async_remote_copy(
            src_ref=stx.at[c], dst_ref=srx.at[c, k], send_sem=st_send.at[c, k], recv_sem=st_recv.at[c, k],
            device_id=(lax.rem(me + k, N_DEV),), device_id_type=MESH)

    def send_stats(c, tg):
        slot = lax.rem(c, 2)
        tm = tmax[slot]
        m_loc = jnp.max(tm, axis=0, keepdims=True)
        s_loc = jnp.sum(tsum[slot] * jnp.exp2((tm - m_loc) * EXP_SCALE), axis=0, keepdims=True)
        stx[c, 0:1, :] = m_loc
        stx[c, 1:2, :] = s_loc
        stx[c, 2:3, :] = jnp.sum(tg, axis=0, keepdims=True)
        for k in range(1, N_DEV):
            stat_copy(c, k).start()

    def recv_stats(c):
        slot = lax.rem(c, 2)
        for k in range(1, N_DEV):
            stat_copy(c, k).wait()
        parts = [stx[c]] + [srx[c, k] for k in range(1, N_DEV)]
        m_all = functools.reduce(jnp.maximum, [p[0:1] for p in parts])
        s_all = functools.reduce(jnp.add, [p[1:2] * jnp.exp2((p[0:1] - m_all) * EXP_SCALE) for p in parts])
        t_all = functools.reduce(jnp.add, [p[2:3] for p in parts])
        mask = mrow[c]
        weight = mask / mask_total
        lossv[...] += mask * (m_all / LOGIT_SCALE + jnp.log(s_all) - t_all / LOGIT_SCALE)
        crow[...] = jnp.exp2((tmax[slot] - m_all) * EXP_SCALE) * (weight / s_all)
        return weight

    def dz_out(c):
        return pltpu.make_async_copy(dzb.at[lax.rem(c, 2)], dz_hbm.at[:, pl.ds(pl.multiple_of(c * CTOK, CTOK), CTOK)], dz_sem.at[lax.rem(c, 2)])

    def dz_rows(c, weight, k):
        slot = lax.rem(c, 2)
        iota = lax.broadcasted_iota(jnp.int32, (DZ_BLOCK, CTOK), 0)
        y = yrow[c]
        s0, n0 = KTILES[k]
        for i, (s, n) in enumerate(TILES):
            if s0 <= s < s0 + n0:
                ci = crow[i:i + 1, :]
                for r in range(s, s + n, DZ_BLOCK):
                    e = ebuf[slot, r:r + DZ_BLOCK, :]
                    dzb[slot, r:r + DZ_BLOCK, :] = (e * ci - jnp.where(iota == (y - r), weight, 0.0)).astype(BF16)

    def dh_mm(c, k, half):
        s, n = KTILES[k]
        cols = slice(half * HALF, half * HALF + HALF)
        part = lax.dot_general(dzb[lax.rem(c, 2), s:s + n, :], emb[s:s + n, cols], (((0,), (0,)), ((), ())), preferred_element_type=F32)
        part = part.reshape(2, 2, 2, PIECE, HALF)
        if k == 0:
            acc[c, :, :, :, :, cols] = part
        else:
            acc[c, :, :, :, :, cols] += part

    def dg_part(c, half):
        cols = slice(half * HALF, half * HALF + HALF)
        total = jnp.zeros((8, HALF), F32)
        for r in range(CTOK // PIECE):
            inv = rcol[c, r][:, 0:1]
            xh = xv[c, r, :, cols].astype(F32) * inv
            total = total + fold8(acc[c, r // 4, (r // 2) % 2, r % 2, :, cols] * xh)
        dgv[:, cols] += jnp.sum(total, axis=0, keepdims=True)

    def rs_copy(c, half, stage):
        cols = pl.ds(half * HALF, HALF)
        if stage == 0:
            src, dst, dev = acc.at[c, :, :, 1 - core, :, cols], ra.at[c, half], peer_core
        elif stage == 1 and half == 0:
            src, dst, dev = acc.at[c, :, 1 - xc, core, :, cols], rb.at[c, half], peer_x
        elif stage == 1:
            src, dst, dev = acc.at[c, 1 - yc, :, core, :, cols], rb.at[c, half], peer_y
        elif half == 0:
            src, dst, dev = acc.at[c, 1 - yc, xc, core, :, cols], rc.at[c, half], peer_y
        else:
            src, dst, dev = acc.at[c, yc, 1 - xc, core, :, cols], rc.at[c, half], peer_x
        return pltpu.make_async_remote_copy(
            src_ref=src, dst_ref=dst, send_sem=rs_send.at[c, half, stage], recv_sem=rs_recv.at[c, half, stage],
            device_id=(dev,), device_id_type=MESH)

    def rs_start(c, half, stage):
        rs_copy(c, half, stage).start()

    def rs_finish(c, half, stage):
        rs_copy(c, half, stage).wait()
        cols = pl.ds(half * HALF, HALF)
        if stage == 0:
            acc[c, :, :, core, :, cols] += ra[c, half]
        elif stage == 1 and half == 0:
            acc[c, :, xc, core, :, cols] += rb[c, half]
        elif stage == 1:
            acc[c, yc, :, core, :, cols] += rb[c, half]
        else:
            acc[c, yc, xc, core, :, cols] += rc[c, half]
        if stage < 2:
            rs_start(c, half, stage + 1)

    def step(s, _):
        lc = jnp.minimum(s, CHUNKS - 1)
        dc = jnp.maximum(s - 1, 0)
        pc = jnp.maximum(s - 2, 0)

        @pl.when(s < CHUNKS)
        def _():
            tgt[...] = logits(lc, 0, N_TILES // 2, jnp.zeros((8, CTOK), F32))

        @pl.when(s == 0)
        def _():
            e_copies[1].wait()
            for c in range(1, CHUNKS):
                x_copies[c].wait()

        @pl.when(jnp.logical_and(s >= 2, s < CHUNKS))
        def _():
            rs_finish(pc, 1, 0)

        @pl.when(s < CHUNKS)
        def _():
            tg = logits(lc, N_TILES // 2, N_TILES, tgt[...])
            send_stats(lc, tg)

        @pl.when(s < CHUNKS - 1)
        def _():
            norm_chunk(s + 1)

        @pl.when(jnp.logical_and(s >= 2, s < CHUNKS))
        def _():
            rs_finish(pc, 0, 1)

        @pl.when(s >= 1)
        def _():
            @pl.when(s >= 3)
            def _():
                dz_out(dc).wait()
            weight = recv_stats(dc)
            dz_rows(dc, weight, 0)
            for k in range(1, len(KTILES)):
                dz_rows(dc, weight, k)
                dh_mm(dc, k - 1, 0)
            dh_mm(dc, len(KTILES) - 1, 0)
            dz_out(dc).start()
            rs_start(dc, 0, 0)
            dg_part(dc, 0)

        @pl.when(jnp.logical_and(s >= 2, s < CHUNKS))
        def _():
            rs_finish(pc, 1, 1)

        @pl.when(s == CHUNKS)
        def _():
            rs_finish(pc, 1, 0)

        @pl.when(s >= 1)
        def _():
            for k in range(len(KTILES)):
                dh_mm(dc, k, 1)
            rs_start(dc, 1, 0)
            rs_finish(dc, 0, 0)
            dg_part(dc, 1)

        @pl.when(jnp.logical_and(s >= 2, s < CHUNKS))
        def _():
            rs_finish(pc, 0, 2)
            rs_finish(pc, 1, 2)
        return 0

    x_copies[0].wait()
    norm_chunk(0)
    pl.semaphore_wait(barrier, N_DEV - 1)
    e_copies[0].wait()
    lax.fori_loop(0, CHUNKS + 1, step, 0)

    def dg_copy(k):
        return pltpu.make_async_remote_copy(
            src_ref=dgv, dst_ref=dgrx.at[k], send_sem=dg_send.at[k], recv_sem=dg_recv.at[k],
            device_id=(lax.rem(me + k, N_DEV),), device_id_type=MESH)

    for k in range(1, N_DEV):
        dg_copy(k).start()
    h_copy = pltpu.make_async_copy(hs, h_hbm, h_sem)
    h_copy.start()
    c2, c3 = CHUNKS - 2, CHUNKS - 1
    rs_finish(c2, 0, 1)
    rs_finish(c3, 1, 0)
    rs_finish(c2, 1, 1)
    rs_finish(c3, 0, 1)
    rs_finish(c3, 1, 1)
    for k in range(1, N_DEV):
        dg_copy(k).wait()
    dg_out[...] = functools.reduce(jnp.add, [dgrx[k] for k in range(1, N_DEV)], dgv[...]) / LOGIT_SCALE
    loss_out[...] = jnp.broadcast_to(jnp.sum(lossv[...], axis=1, keepdims=True) / mask_total, loss_out.shape)
    rs_finish(c2, 0, 2)
    rs_finish(c2, 1, 2)
    rs_finish(c3, 0, 2)
    rs_finish(c3, 1, 2)
    for c in range(CHUNKS):
        dh = acc[c, yc, xc, core] / LOGIT_SCALE
        piece = core + 2 * xc + 4 * yc
        inv = rcol[c, piece][:, 0:1]
        xh = xv[c, piece].astype(F32) * inv
        u = dh * g_in[...]
        dx_out[c * PIECE:(c + 1) * PIECE, :] = inv * (u - xh * jnp.mean(u * xh, axis=1, keepdims=True))
    h_copy.wait()
    dz_out(c2).wait()
    dz_out(c3).wait()


def table_grad_kernel(dz, h, dx_in, dg_in, loss_in, de_out, dx_out, dg_out, loss_out):
    de_out[...] = jnp.dot(dz[...], h[...], preferred_element_type=F32) * (1.0 / LOGIT_SCALE)

    @pl.when(pl.program_id(0) == 0)
    def _():
        dx_out[...] = dx_in[...]
        dg_out[...] = dg_in[...]
        loss_out[...] = loss_in[...]


def solution(mesh):
    vp_axis = mesh.axis_names[0]
    vmem = pl.BlockSpec(memory_space=pltpu.VMEM)
    anywhere = pl.BlockSpec(memory_space=pl.ANY)
    dma = pltpu.SemaphoreType.DMA

    def local_step(residual, labels, loss_mask, norm_gain, table_shard):
        max_tile = max(n for _, n in TILES)
        dz, h, dx, dg, loss = pl.pallas_call(
            main_kernel,
            out_shape=(
                jax.ShapeDtypeStruct((ROWS, TOKENS), BF16),
                jax.ShapeDtypeStruct((CHUNKS, CTOK, DIM), BF16),
                jax.ShapeDtypeStruct((TOKENS // N_DEV, DIM), F32),
                jax.ShapeDtypeStruct((1, DIM), F32),
                jax.ShapeDtypeStruct((1, 128), F32),
            ),
            in_specs=[anywhere, vmem, vmem, vmem, anywhere],
            out_specs=(anywhere, anywhere, vmem, vmem, vmem),
            scratch_shapes=[
                pltpu.VMEM((ROWS, DIM), BF16),
                pltpu.VMEM((CHUNKS, N_DEV, PIECE, DIM), BF16),
                pltpu.VMEM((CHUNKS, CTOK, DIM), BF16),
                pltpu.VMEM((CHUNKS, DIM, CTOK), BF16),
                pltpu.VMEM((CHUNKS, N_DEV, PIECE, 128), F32),
                pltpu.VMEM((2, ROWS, CTOK), F32),
                pltpu.VMEM((2, ROWS, CTOK), BF16),
                pltpu.VMEM((CHUNKS, 2, 2, 2, PIECE, DIM), F32),
                pltpu.VMEM((max_tile, CTOK), F32),
                pltpu.VMEM((max_tile, CTOK), F32),
                pltpu.VMEM((CHUNKS, 1, CTOK), jnp.int32),
                pltpu.VMEM((CHUNKS, 1, CTOK), F32),
                pltpu.VMEM((2, N_TILES, CTOK), F32),
                pltpu.VMEM((2, N_TILES, CTOK), F32),
                pltpu.VMEM((N_TILES, CTOK), F32),
                pltpu.VMEM((8, CTOK), F32),
                pltpu.VMEM((CHUNKS, 8, CTOK), F32),
                pltpu.VMEM((CHUNKS, N_DEV, 8, CTOK), F32),
                pltpu.VMEM((1, CTOK), F32),
                pltpu.VMEM((1, DIM), F32),
                pltpu.VMEM((N_DEV, 1, DIM), F32),
                pltpu.VMEM((CHUNKS, 2, 2, 2, PIECE, HALF), F32),
                pltpu.VMEM((CHUNKS, 2, 2, PIECE, HALF), F32),
                pltpu.VMEM((CHUNKS, 2, PIECE, HALF), F32),
                dma((6,)),
                dma,
                dma((2,)),
                dma((CHUNKS, N_DEV)),
                dma((CHUNKS, N_DEV)),
                dma((CHUNKS, 2, 3)),
                dma((CHUNKS, 2, 3)),
                dma((N_DEV,)),
                dma((N_DEV,)),
            ],
            compiler_params=pltpu.CompilerParams(collective_id=0, has_side_effects=True, vmem_limit_bytes=60 << 20),
            cost_estimate=pl.CostEstimate(flops=4 * ROWS * TOKENS * DIM, bytes_accessed=30 << 20, transcendentals=ROWS * TOKENS),
        )(
            residual.reshape(N_DEV, CHUNKS, PIECE, DIM),
            labels.reshape(N_DEV, 128),
            loss_mask.reshape(N_DEV, 128),
            norm_gain.reshape(1, DIM),
            table_shard,
        )
        block = 784
        whole = lambda shape: pl.BlockSpec(shape, lambda i: (0, 0))
        d_embed, dx, dg, loss = pl.pallas_call(
            table_grad_kernel,
            grid=(pl.cdiv(ROWS, block),),
            out_shape=(
                jax.ShapeDtypeStruct((ROWS, DIM), F32),
                jax.ShapeDtypeStruct(dx.shape, F32),
                jax.ShapeDtypeStruct(dg.shape, F32),
                jax.ShapeDtypeStruct(loss.shape, F32),
            ),
            in_specs=[pl.BlockSpec((block, TOKENS), lambda i: (i, 0)), whole((TOKENS, DIM)), whole(dx.shape), whole(dg.shape), whole(loss.shape)],
            out_specs=(pl.BlockSpec((block, DIM), lambda i: (i, 0)), whole(dx.shape), whole(dg.shape), whole(loss.shape)),
            compiler_params=pltpu.CompilerParams(vmem_limit_bytes=60 << 20),
            cost_estimate=pl.CostEstimate(flops=2 * ROWS * TOKENS * DIM, bytes_accessed=40 << 20, transcendentals=0),
        )(dz, h.reshape(TOKENS, DIM), dx, dg, loss)
        return loss[0, 0], dx, d_embed, dg[0]

    return jax.shard_map(local_step, mesh=mesh, in_specs=(P(), P(), P(), P(), P(vp_axis, None)), out_specs=(P(), P(vp_axis, None), P(vp_axis, None), P()), check_vma=False)
```

```python
import functools

import jax
import jax.numpy as jnp
from jax import lax
from jax.experimental import pallas as pl
from jax.experimental.pallas import tpu as pltpu
from jax.sharding import PartitionSpec as P

VOCAB_REAL = 49155
LOGIT_SCALE = 6.0
NORM_EPS = 1e-6
LOG2E = 1.4426950408889634
F32 = jnp.float32
BF16 = jnp.bfloat16
MESH = pl.DeviceIdType.MESH

N_DEV = 8
TOKENS = 1024
DIM = 1024
ROWS = 6176
CHUNKS = 4
CTOK = 256
PIECE = 32
HALF = DIM // 2
L_TILE = 256
K_TILE = 1024
DZ_BLOCK = 32
L_BLOCK = 16
MASK_FROM = VOCAB_REAL - (N_DEV - 1) * ROWS
EXP_SCALE = LOG2E / LOGIT_SCALE


def split_rows(step):
    cuts = [[i * step, step] for i in range(ROWS // step)]
    cuts[-1][1] = ROWS - cuts[-1][0]
    return [tuple(c) for c in cuts]


TILES = split_rows(L_TILE)
KTILES = split_rows(K_TILE)
N_TILES = len(TILES)
E_SPLIT = (0, 3, 8, 16)
EARLY = 2
LATE_ROWS = (CHUNKS - EARLY) * PIECE


def fold8(v):
    return jnp.sum(v.reshape(v.shape[0] // 8, 8, v.shape[1]), axis=0)


def interleave(main, side, ratio):
    main_done = side_done = False
    while not (main_done and side_done):
        if not main_done:
            main_done = next(main, 0) == 0
        for _ in range(ratio):
            if not side_done:
                side_done = next(side, 0) == 0


def main_kernel(x_hbm, y_in, m_in, g_in, e_hbm,
                dz_hbm, h_hbm, own_out, sx_out, sy_out, sd_out, dg_out, loss_out,
                emb, xv, hs, ht, rcol, ebuf, dzb, acc, ub0, ub1, yrow, mrow,
                tmax, tsum, crow, tgt, stx, srx, lossv, dgv, dgsend, dgrx, ra, rb, rc,
                in_sem, h_sem, dz_sem, st_send, st_recv, rs_send, rs_recv, dg_send, dg_recv):
    me = lax.axis_index("vp")
    core = lax.rem(me, 2)
    xc = lax.rem(me // 2, 2)
    yc = me // 4
    peer_core = me + 1 - 2 * core
    peer_x = me + 2 - 4 * xc
    peer_y = me + 4 - 8 * yc

    e_cuts = [TILES[t][0] for t in E_SPLIT] + [ROWS]
    e_copies = [
        pltpu.make_async_copy(e_hbm.at[pl.ds(a, b - a)], emb.at[pl.ds(a, b - a)], in_sem.at[CHUNKS + j])
        for j, (a, b) in enumerate(zip(e_cuts[:-1], e_cuts[1:]))
    ]
    x_copies = [pltpu.make_async_copy(x_hbm.at[:, c], xv.at[c], in_sem.at[c]) for c in range(CHUNKS)]
    x_copies[0].start()
    for copy in e_copies:
        copy.start()
    for c in range(1, CHUNKS):
        x_copies[c].start()

    barrier = pltpu.get_barrier_semaphore()
    for k in range(1, N_DEV):
        pl.semaphore_signal(barrier, inc=1, device_id=(lax.rem(me + k, N_DEV),), device_id_type=MESH)

    lane = lax.broadcasted_iota(jnp.int32, (1, 128), 1) // PIECE
    base = me * ROWS
    for c in range(CHUNKS):
        for half in range(2):
            yh = jnp.zeros((1, 128), jnp.int32)
            mh = jnp.zeros((1, 128), F32)
            for i in range(4):
                row = half * 4 + i
                shift = (PIECE * (i - c)) % 128
                yr, mr = y_in[row:row + 1, :], m_in[row:row + 1, :]
                if shift:
                    yr, mr = pltpu.roll(yr, shift, 1), pltpu.roll(mr, shift, 1)
                yh = jnp.where(lane == i, yr, yh)
                mh = jnp.where(lane == i, mr, mh)
            yrow[c, :, half * 128:half * 128 + 128] = yh - base
            mrow[c, :, half * 128:half * 128 + 128] = mh
    mask_total = jnp.sum(jnp.sum(m_in[...], axis=0, keepdims=True), axis=1, keepdims=True)
    lossv[...] = jnp.zeros_like(lossv)
    dgv[...] = jnp.zeros_like(dgv)
    limit = VOCAB_REAL - base

    def norm_chunk(c):
        g = g_in[...]
        for r in range(CTOK // PIECE):
            xf = xv[c, r].astype(F32)
            inv = lax.rsqrt(jnp.mean(xf * xf, axis=1, keepdims=True) + NORM_EPS)
            rcol[c, r] = jnp.broadcast_to(inv, (PIECE, 128))
            hs[c, r * PIECE:(r + 1) * PIECE, :] = (xf * inv * g).astype(BF16)
        ht[c] = hs[c].T

    def logits(c, lo, hi, tg, before=None):
        slot = lax.rem(c, 2)
        iota = lax.broadcasted_iota(jnp.int32, (L_BLOCK, CTOK), 0)
        y = yrow[c]
        eb = ebuf.at[slot]
        ubs = (ub0, ub1)
        state = [tg]

        def mm(i):
            s, n = TILES[i]
            ubs[i % 2][0:n, :] = jnp.dot(emb[s:s + n, :], ht[c], preferred_element_type=F32)
            yield 1

        def post(i):
            s, n = TILES[i]
            u_ref = ubs[i % 2]
            top = jnp.full((L_BLOCK, CTOK), -jnp.inf, F32)
            for r in range(0, n, L_BLOCK):
                u = u_ref[r:r + L_BLOCK, :]
                if s + r + L_BLOCK > MASK_FROM:
                    u = jnp.where(iota < limit - (s + r), u, -jnp.inf)
                    u_ref[r:r + L_BLOCK, :] = u
                top = jnp.maximum(top, u)
            m = jnp.max(top, axis=0, keepdims=True)
            s8 = jnp.zeros((L_BLOCK, CTOK), F32)
            for r in range(0, n, L_BLOCK):
                u = u_ref[r:r + L_BLOCK, :]
                e = jnp.exp2((u - m) * EXP_SCALE)
                eb[s + r:s + r + L_BLOCK, :] = e
                s8 = s8 + e
                state[0] = state[0] + jnp.where(iota == (y - (s + r)), u, 0.0)
                if r % 64 == 64 - L_BLOCK:
                    yield 1
            tmax[slot, i:i + 1, :] = m
            tsum[slot, i:i + 1, :] = jnp.sum(s8, axis=0, keepdims=True)
            yield 1

        for _ in mm(lo):
            pass
        for i in range(lo + 1, hi):
            if before is not None and i in before:
                before[i]()
            interleave(mm(i), post(i - 1), 6)
        for _ in post(hi - 1):
            pass
        return state[0]

    def stat_copy(c, k):
        return pltpu.make_async_remote_copy(
            src_ref=stx.at[c], dst_ref=srx.at[c, k], send_sem=st_send.at[c, k], recv_sem=st_recv.at[c, k],
            device_id=(lax.rem(me + k, N_DEV),), device_id_type=MESH)

    def send_stats(c, tg):
        slot = lax.rem(c, 2)
        tm = tmax[slot]
        m_loc = jnp.max(tm, axis=0, keepdims=True)
        s_loc = jnp.sum(tsum[slot] * jnp.exp2((tm - m_loc) * EXP_SCALE), axis=0, keepdims=True)
        stx[c, 0:1, :] = m_loc
        stx[c, 1:2, :] = s_loc
        stx[c, 2:3, :] = jnp.sum(tg, axis=0, keepdims=True)
        for k in range(1, N_DEV):
            stat_copy(c, k).start()

    def recv_stats(c):
        slot = lax.rem(c, 2)
        for k in range(1, N_DEV):
            stat_copy(c, k).wait()
        parts = [stx[c]] + [srx[c, k] for k in range(1, N_DEV)]
        m_all = functools.reduce(jnp.maximum, [p[0:1] for p in parts])
        s_all = functools.reduce(jnp.add, [p[1:2] * jnp.exp2((p[0:1] - m_all) * EXP_SCALE) for p in parts])
        t_all = functools.reduce(jnp.add, [p[2:3] for p in parts])
        mask = mrow[c]
        weight = mask / mask_total
        lossv[...] += mask * (m_all / LOGIT_SCALE + jnp.log(s_all) - t_all / LOGIT_SCALE)
        crow[...] = jnp.exp2((tmax[slot] - m_all) * EXP_SCALE) * (weight / s_all)
        return weight

    def dz_out(c):
        return pltpu.make_async_copy(dzb.at[lax.rem(c, 2)], dz_hbm.at[:, pl.ds(pl.multiple_of(c * CTOK, CTOK), CTOK)], dz_sem.at[lax.rem(c, 2)])

    def dz_rows(c, weight, k):
        slot = lax.rem(c, 2)
        iota = lax.broadcasted_iota(jnp.int32, (DZ_BLOCK, CTOK), 0)
        y = yrow[c]
        s0, n0 = KTILES[k]
        for i, (s, n) in enumerate(TILES):
            if s0 <= s < s0 + n0:
                ci = crow[i:i + 1, :]
                for r in range(s, s + n, DZ_BLOCK):
                    e = ebuf[slot, r:r + DZ_BLOCK, :]
                    dzb[slot, r:r + DZ_BLOCK, :] = (e * ci - jnp.where(iota == (y - r), weight, 0.0)).astype(BF16)

    def dh_mm(c, k, half):
        s, n = KTILES[k]
        cols = slice(half * HALF, half * HALF + HALF)
        part = lax.dot_general(dzb[lax.rem(c, 2), s:s + n, :], emb[s:s + n, cols], (((0,), (0,)), ((), ())), preferred_element_type=F32)
        part = part.reshape(2, 2, 2, PIECE, HALF)
        if k == 0:
            acc[c, :, :, :, :, cols] = part
        else:
            acc[c, :, :, :, :, cols] += part

    def dg_part(c, half):
        cols = slice(half * HALF, half * HALF + HALF)
        total = jnp.zeros((8, HALF), F32)
        for r in range(CTOK // PIECE):
            inv = rcol[c, r][:, 0:1]
            xh = xv[c, r, :, cols].astype(F32) * inv
            total = total + fold8(acc[c, r // 4, (r // 2) % 2, r % 2, :, cols] * xh)
        dgv[:, cols] += jnp.sum(total, axis=0, keepdims=True)

    def rs_copy(c, half, stage):
        cols = pl.ds(half * HALF, HALF)
        if stage == 0:
            src, dst, dev = acc.at[c, :, :, 1 - core, :, cols], ra.at[c, half], peer_core
        elif stage == 1 and half == 0:
            src, dst, dev = acc.at[c, :, 1 - xc, core, :, cols], rb.at[c, half], peer_x
        elif stage == 1:
            src, dst, dev = acc.at[c, 1 - yc, :, core, :, cols], rb.at[c, half], peer_y
        elif half == 0:
            src, dst, dev = acc.at[c, 1 - yc, xc, core, :, cols], rc.at[c, half], peer_y
        else:
            src, dst, dev = acc.at[c, yc, 1 - xc, core, :, cols], rc.at[c, half], peer_x
        return pltpu.make_async_remote_copy(
            src_ref=src, dst_ref=dst, send_sem=rs_send.at[c, half, stage], recv_sem=rs_recv.at[c, half, stage],
            device_id=(dev,), device_id_type=MESH)

    def rs_start(c, half, stage):
        rs_copy(c, half, stage).start()

    def rs_finish(c, half, stage):
        rs_copy(c, half, stage).wait()
        cols = pl.ds(half * HALF, HALF)
        if stage == 0:
            acc[c, :, :, core, :, cols] += ra[c, half]
        elif stage == 1 and half == 0:
            acc[c, :, xc, core, :, cols] += rb[c, half]
        elif stage == 1:
            acc[c, yc, :, core, :, cols] += rb[c, half]
        else:
            acc[c, yc, xc, core, :, cols] += rc[c, half]
        if stage < 2:
            rs_start(c, half, stage + 1)

    def pair_finish(c, half):
        rs_copy(c, half, 0).wait()
        cols = slice(half * HALF, half * HALF + HALF)
        late = pl.ds(pl.multiple_of((c - EARLY) * PIECE, PIECE), PIECE)
        mine = pl.ds(pl.multiple_of(c * PIECE, PIECE), PIECE)

        def pair_sum(y, x):
            return acc[c, y, x, core, :, cols] + ra[c, half, y, x]

        own_out[mine, cols] = pair_sum(yc, xc)
        sx_out[late, cols] = pair_sum(yc, 1 - xc)
        sy_out[late, cols] = pair_sum(1 - yc, xc)
        sd_out[late, cols] = pair_sum(1 - yc, 1 - xc)

    def step(s, _):
        lc = jnp.minimum(s, CHUNKS - 1)
        dc = s - 1
        pc = jnp.maximum(s - 2, 0)

        @pl.when(s < CHUNKS)
        def _():
            tgt[...] = logits(lc, 0, N_TILES // 2, jnp.zeros((L_BLOCK, CTOK), F32))

        @pl.when(jnp.logical_and(s >= 2, s < CHUNKS))
        def _():
            rs_finish(pc, 1, 0)

        @pl.when(s < CHUNKS)
        def _():
            tg = logits(lc, N_TILES // 2, N_TILES, tgt[...])
            send_stats(lc, tg)

        @pl.when(s == 3)
        def _():
            rs_finish(0, 0, 2)
            rs_finish(0, 1, 2)

        @pl.when(s >= 3)
        def _():
            dz_out(dc).wait()

        weight = recv_stats(dc)
        dz_rows(dc, weight, 0)
        for k in range(1, len(KTILES)):
            dz_rows(dc, weight, k)
            dh_mm(dc, k - 1, 0)
        dh_mm(dc, len(KTILES) - 1, 0)
        dz_out(dc).start()
        rs_start(dc, 0, 0)
        dg_part(dc, 0)

        @pl.when(jnp.logical_and(s >= 2, s < CHUNKS))
        def _():
            rs_finish(pc, 0, 1)

        @pl.when(s == CHUNKS)
        def _():
            pair_finish(CHUNKS - 2, 1)
            rs_finish(1, 0, 2)

        for k in range(len(KTILES)):
            dh_mm(dc, k, 1)
        rs_start(dc, 1, 0)
        dg_part(dc, 1)

        @pl.when(dc < EARLY)
        def _():
            rs_finish(dc, 0, 0)

        @pl.when(dc >= EARLY)
        def _():
            pair_finish(dc, 0)

        @pl.when(jnp.logical_and(s >= 2, s < CHUNKS))
        def _():
            rs_finish(pc, 1, 1)
        return 0

    x_copies[0].wait()
    norm_chunk(0)
    e_copies[0].wait()

    def more_rows(j):
        def run():
            e_copies[j].wait()
        return run

    tg0 = logits(0, 0, N_TILES, jnp.zeros((L_BLOCK, CTOK), F32), {E_SPLIT[j]: more_rows(j) for j in range(1, len(E_SPLIT))})
    pl.semaphore_wait(barrier, N_DEV - 1)
    send_stats(0, tg0)
    for c in range(1, CHUNKS):
        x_copies[c].wait()
        norm_chunk(c)
    h_copy = pltpu.make_async_copy(hs, h_hbm, h_sem)
    h_copy.start()
    lax.fori_loop(1, CHUNKS + 1, step, 0)

    dgsend[...] = dgv[...]
    dg_copy = pltpu.make_async_remote_copy(
        src_ref=dgsend, dst_ref=dgrx, send_sem=dg_send, recv_sem=dg_recv, device_id=(peer_core,), device_id_type=MESH)
    dg_copy.start()
    loss_out[...] = jnp.broadcast_to(jnp.sum(lossv[...], axis=1, keepdims=True) / mask_total, loss_out.shape)
    rs_finish(1, 1, 2)
    for c in range(EARLY):
        own_out[c * PIECE:(c + 1) * PIECE, :] = acc[c, yc, xc, core]
    pair_finish(CHUNKS - 1, 1)
    dg_copy.wait()
    dg_pair = dgv[...] + dgrx[...]
    dg_out[...] = dg_pair
    for out in (sx_out, sy_out, sd_out):
        out[LATE_ROWS:LATE_ROWS + 8, :] = jnp.broadcast_to(dg_pair, (8, DIM))
    h_copy.wait()
    dz_out(CHUNKS - 2).wait()
    dz_out(CHUNKS - 1).wait()


def norm_grad_kernel(own, rx, ry, rd, dg_pair, g_in, x_hbm, dx_out, dg_out, x, sem):
    copy = pltpu.make_async_copy(x_hbm.at[lax.axis_index("vp")], x, sem)
    copy.start()
    dg_out[...] = (dg_pair[...] + rx[LATE_ROWS:LATE_ROWS + 1, :] + ry[LATE_ROWS:LATE_ROWS + 1, :] + rd[LATE_ROWS:LATE_ROWS + 1, :]) / LOGIT_SCALE
    copy.wait()
    for c in range(CHUNKS):
        rows = slice(c * PIECE, (c + 1) * PIECE)
        dh = own[rows, :]
        if c >= EARLY:
            late = slice((c - EARLY) * PIECE, (c - EARLY + 1) * PIECE)
            dh = dh + rx[late, :] + ry[late, :] + rd[late, :]
        xf = x[rows, :].astype(F32)
        inv = lax.rsqrt(jnp.mean(xf * xf, axis=1, keepdims=True) + NORM_EPS)
        xh = xf * inv
        u = dh / LOGIT_SCALE * g_in[...]
        dx_out[rows, :] = inv * (u - xh * jnp.mean(u * xh, axis=1, keepdims=True))


D_FIRST, D_STEP, D_RING = 256, 768, 3
D_LOOPS = (ROWS - D_FIRST) // D_STEP
D_REST = ROWS - D_FIRST - D_LOOPS * D_STEP


def table_grad_kernel(dz_hbm, h_hbm, de_hbm, dz, h, ring, in_sem, h_sem, out_sem):
    tail = D_LOOPS + 1
    tail_row = ROWS - D_REST

    def fetch(i, row, rows):
        return pltpu.make_async_copy(dz_hbm.at[pl.ds(row, rows)], dz.at[pl.ds(row, rows)], in_sem.at[i])

    def store(slot, row, rows):
        return pltpu.make_async_copy(ring.at[slot, pl.ds(0, rows)], de_hbm.at[pl.ds(row, rows)], out_sem.at[slot])

    def row_of(i):
        return pl.multiple_of(D_FIRST + (i - 1) * D_STEP, 16)

    def tile(slot, row, rows):
        ring[slot, 0:rows, :] = jnp.dot(dz[pl.ds(row, rows), :], h[...], preferred_element_type=F32) * (1.0 / LOGIT_SCALE)
        store(slot, row, rows).start()

    h_copy = pltpu.make_async_copy(h_hbm, h, h_sem)
    fetch(0, 0, D_FIRST).start()
    h_copy.start()
    for i in (1, 2):
        fetch(i, D_FIRST + (i - 1) * D_STEP, D_STEP).start()
    h_copy.wait()
    fetch(0, 0, D_FIRST).wait()
    tile(0, 0, D_FIRST)

    def body(i, _):
        slot = lax.rem(i, D_RING)
        fetch(i, row_of(i), D_STEP).wait()

        @pl.when(i + 2 <= D_LOOPS)
        def _():
            fetch(i + 2, row_of(i + 2), D_STEP).start()

        @pl.when(i == D_LOOPS - 1)
        def _():
            fetch(tail, tail_row, D_REST).start()

        @pl.when(i == D_RING)
        def _():
            store(slot, 0, D_FIRST).wait()

        @pl.when(i > D_RING)
        def _():
            store(slot, 0, D_STEP).wait()

        tile(slot, row_of(i), D_STEP)
        return 0

    lax.fori_loop(1, D_LOOPS + 1, body, 0)
    fetch(tail, tail_row, D_REST).wait()
    store(tail % D_RING, 0, D_STEP).wait()
    tile(tail % D_RING, tail_row, D_REST)
    for i in range(tail - D_RING + 1, tail):
        store(i % D_RING, 0, D_STEP).wait()
    store(tail % D_RING, 0, D_REST).wait()


def solution(mesh):
    vp_axis = mesh.axis_names[0]
    vmem = pl.BlockSpec(memory_space=pltpu.VMEM)
    anywhere = pl.BlockSpec(memory_space=pl.ANY)
    dma = pltpu.SemaphoreType.DMA

    def local_step(residual, labels, loss_mask, norm_gain, table_shard):
        max_tile = max(n for _, n in TILES)
        dz, h, own, sx, sy, sd, dg_pair, loss = pl.pallas_call(
            main_kernel,
            out_shape=(
                jax.ShapeDtypeStruct((ROWS, TOKENS), BF16),
                jax.ShapeDtypeStruct((CHUNKS, CTOK, DIM), BF16),
                jax.ShapeDtypeStruct((TOKENS // N_DEV, DIM), F32),
                *[jax.ShapeDtypeStruct((LATE_ROWS + 8, DIM), F32)] * 3,
                jax.ShapeDtypeStruct((1, DIM), F32),
                jax.ShapeDtypeStruct((1, 128), F32),
            ),
            in_specs=[anywhere, vmem, vmem, vmem, anywhere],
            out_specs=(anywhere, anywhere, vmem, vmem, vmem, vmem, vmem, vmem),
            scratch_shapes=[
                pltpu.VMEM((ROWS, DIM), BF16),
                pltpu.VMEM((CHUNKS, N_DEV, PIECE, DIM), BF16),
                pltpu.VMEM((CHUNKS, CTOK, DIM), BF16),
                pltpu.VMEM((CHUNKS, DIM, CTOK), BF16),
                pltpu.VMEM((CHUNKS, N_DEV, PIECE, 128), F32),
                pltpu.VMEM((2, ROWS, CTOK), F32),
                pltpu.VMEM((2, ROWS, CTOK), BF16),
                pltpu.VMEM((CHUNKS, 2, 2, 2, PIECE, DIM), F32),
                pltpu.VMEM((max_tile, CTOK), F32),
                pltpu.VMEM((max_tile, CTOK), F32),
                pltpu.VMEM((CHUNKS, 1, CTOK), jnp.int32),
                pltpu.VMEM((CHUNKS, 1, CTOK), F32),
                pltpu.VMEM((2, N_TILES, CTOK), F32),
                pltpu.VMEM((2, N_TILES, CTOK), F32),
                pltpu.VMEM((N_TILES, CTOK), F32),
                pltpu.VMEM((L_BLOCK, CTOK), F32),
                pltpu.VMEM((CHUNKS, 8, CTOK), F32),
                pltpu.VMEM((CHUNKS, N_DEV, 8, CTOK), F32),
                pltpu.VMEM((1, CTOK), F32),
                pltpu.VMEM((1, DIM), F32),
                pltpu.VMEM((1, DIM), F32),
                pltpu.VMEM((1, DIM), F32),
                pltpu.VMEM((CHUNKS, 2, 2, 2, PIECE, HALF), F32),
                pltpu.VMEM((EARLY, 2, 2, PIECE, HALF), F32),
                pltpu.VMEM((EARLY, 2, PIECE, HALF), F32),
                dma((CHUNKS + len(E_SPLIT),)),
                dma,
                dma((2,)),
                dma((CHUNKS, N_DEV)),
                dma((CHUNKS, N_DEV)),
                dma((CHUNKS, 2, 3)),
                dma((CHUNKS, 2, 3)),
                dma,
                dma,
            ],
            compiler_params=pltpu.CompilerParams(collective_id=0, has_side_effects=True, vmem_limit_bytes=60 << 20),
            cost_estimate=pl.CostEstimate(flops=4 * ROWS * TOKENS * DIM, bytes_accessed=30 << 20, transcendentals=ROWS * TOKENS),
        )(
            residual.reshape(N_DEV, CHUNKS, PIECE, DIM),
            labels.reshape(N_DEV, 128),
            loss_mask.reshape(N_DEV, 128),
            norm_gain.reshape(1, DIM),
            table_shard,
        )
        rx, ry, rd = (lax.ppermute(v, vp_axis, [(i, i ^ k) for i in range(N_DEV)]) for v, k in ((sx, 2), (sy, 4), (sd, 6)))
        d_embed = pl.pallas_call(
            table_grad_kernel,
            out_shape=jax.ShapeDtypeStruct((ROWS, DIM), F32),
            in_specs=[anywhere, anywhere],
            out_specs=anywhere,
            scratch_shapes=[
                pltpu.VMEM((ROWS, TOKENS), BF16),
                pltpu.VMEM((TOKENS, DIM), BF16),
                pltpu.VMEM((D_RING, D_STEP, DIM), F32),
                dma((D_LOOPS + 2,)),
                dma,
                dma((D_RING,)),
            ],
            compiler_params=pltpu.CompilerParams(vmem_limit_bytes=60 << 20),
            cost_estimate=pl.CostEstimate(flops=2 * ROWS * TOKENS * DIM, bytes_accessed=40 << 20, transcendentals=0),
        )(dz, h.reshape(TOKENS, DIM))
        own_rows = TOKENS // N_DEV
        dx, dg = pl.pallas_call(
            norm_grad_kernel,
            out_shape=(jax.ShapeDtypeStruct((own_rows, DIM), F32), jax.ShapeDtypeStruct((1, DIM), F32)),
            in_specs=[vmem] * 6 + [anywhere],
            out_specs=(vmem, vmem),
            scratch_shapes=[pltpu.VMEM((own_rows, DIM), BF16), dma],
            compiler_params=pltpu.CompilerParams(vmem_limit_bytes=6 << 20),
            cost_estimate=pl.CostEstimate(flops=20 * own_rows * DIM, bytes_accessed=2 << 20, transcendentals=own_rows),
        )(own, rx, ry, rd, dg_pair, norm_gain.reshape(1, DIM), residual.reshape(N_DEV, own_rows, DIM))
        return loss[0, 0], dx, d_embed, dg[0]

    return jax.shard_map(local_step, mesh=mesh, in_specs=(P(), P(), P(), P(), P(vp_axis, None)), out_specs=(P(), P(vp_axis, None), P(vp_axis, None), P()), check_vma=False)
```

```python
import functools

import jax
import jax.numpy as jnp
from jax import lax
from jax.experimental import pallas as pl
from jax.experimental.pallas import tpu as pltpu
from jax.sharding import PartitionSpec as P

VOCAB_REAL = 49155
LOGIT_SCALE = 6.0
NORM_EPS = 1e-6
LOG2E = 1.4426950408889634
F32 = jnp.float32
BF16 = jnp.bfloat16
MESH = pl.DeviceIdType.MESH

N_DEV = 8
TOKENS = 1024
DIM = 1024
ROWS = 6176
CHUNKS = 4
CTOK = 256
PIECE = 32
HALF = DIM // 2
L_TILE = 128
K_TILE = 1024
DZ_BLOCK = 32
L_BLOCK = 16
LOWEST = float(jnp.finfo(jnp.float32).min)
MASK_FROM = VOCAB_REAL - (N_DEV - 1) * ROWS
EXP_SCALE = LOG2E / LOGIT_SCALE


def split_rows(step):
    cuts = [[i * step, step] for i in range(ROWS // step)]
    cuts[-1][1] = ROWS - cuts[-1][0]
    return [tuple(c) for c in cuts]


TILES = [(i * L_TILE, L_TILE) for i in range(ROWS // L_TILE)] + [(ROWS // L_TILE * L_TILE, ROWS % L_TILE)]
KTILES = split_rows(K_TILE)
N_TILES = len(TILES)
E_SPLIT = (0, 6, 16, 32)
EARLY = 2
LATE_ROWS = (CHUNKS - EARLY) * PIECE


def fold8(v):
    return jnp.sum(v.reshape(v.shape[0] // 8, 8, v.shape[1]), axis=0)


def interleave(main, side, ratio):
    main_done = side_done = False
    while not (main_done and side_done):
        if not main_done:
            main_done = next(main, 0) == 0
        for _ in range(ratio):
            if not side_done:
                side_done = next(side, 0) == 0


def main_kernel(x_hbm, y_in, m_in, g_in, e_hbm,
                dz_hbm, h_hbm, own_out, sx_out, sy_out, sd_out, dg_out, loss_out,
                emb, xv, hs, ht, rcol, ebuf, dzb, acc, ub0, ub1, yrow, mrow,
                tmax, tsum, crow, stx, srx, lossv, dgv, dgsend, dgrx, ra, rb, rc,
                in_sem, h_sem, dz_sem, st_send, st_recv, rs_send, rs_recv, dg_send, dg_recv):
    me = lax.axis_index("vp")
    core = lax.rem(me, 2)
    xc = lax.rem(me // 2, 2)
    yc = me // 4
    peer_core = me + 1 - 2 * core
    peer_x = me + 2 - 4 * xc
    peer_y = me + 4 - 8 * yc

    e_cuts = [TILES[t][0] for t in E_SPLIT] + [ROWS]
    e_copies = [
        pltpu.make_async_copy(e_hbm.at[pl.ds(a, b - a)], emb.at[pl.ds(a, b - a)], in_sem.at[CHUNKS + j])
        for j, (a, b) in enumerate(zip(e_cuts[:-1], e_cuts[1:]))
    ]
    x_copies = [pltpu.make_async_copy(x_hbm.at[:, c], xv.at[c], in_sem.at[c]) for c in range(CHUNKS)]
    x_copies[0].start()
    for copy in e_copies:
        copy.start()
    for c in range(1, CHUNKS):
        x_copies[c].start()

    barrier = pltpu.get_barrier_semaphore()
    for k in range(1, N_DEV):
        pl.semaphore_signal(barrier, inc=1, device_id=(lax.rem(me + k, N_DEV),), device_id_type=MESH)

    lane = lax.broadcasted_iota(jnp.int32, (1, 128), 1) // PIECE
    base = me * ROWS
    for c in range(CHUNKS):
        for half in range(2):
            yh = jnp.zeros((1, 128), jnp.int32)
            mh = jnp.zeros((1, 128), F32)
            for i in range(4):
                row = half * 4 + i
                shift = (PIECE * (i - c)) % 128
                yr, mr = y_in[row:row + 1, :], m_in[row:row + 1, :]
                if shift:
                    yr, mr = pltpu.roll(yr, shift, 1), pltpu.roll(mr, shift, 1)
                yh = jnp.where(lane == i, yr, yh)
                mh = jnp.where(lane == i, mr, mh)
            yrow[c, :, half * 128:half * 128 + 128] = yh - base
            mrow[c, :, half * 128:half * 128 + 128] = mh
    mask_total = jnp.sum(jnp.sum(m_in[...], axis=0, keepdims=True), axis=1, keepdims=True)
    lossv[...] = jnp.zeros_like(lossv)
    dgv[...] = jnp.zeros_like(dgv)
    limit = VOCAB_REAL - base

    def norm_rows(c, r):
        xf = xv[c, r].astype(F32)
        inv = lax.rsqrt(jnp.mean(xf * xf, axis=1, keepdims=True) + NORM_EPS)
        rcol[c, r] = jnp.broadcast_to(inv, (PIECE, 128))
        hs[c, r * PIECE:(r + 1) * PIECE, :] = (xf * inv * g_in[...]).astype(BF16)

    def norm_chunk(c):
        for r in range(CTOK // PIECE):
            norm_rows(c, r)
        ht[c] = hs[c].T

    def logits(c, lo, hi, tg, before=None):
        slot = lax.rem(c, 2)
        iota = lax.broadcasted_iota(jnp.int32, (L_BLOCK, CTOK), 0)
        y = yrow[c]
        eb = ebuf.at[slot]
        ubs = (ub0, ub1)
        state = [tg]

        def mm(i):
            s, n = TILES[i]
            ubs[i % 2][0:n, :] = jnp.dot(emb[s:s + n, :], ht[c], preferred_element_type=F32)
            yield 1

        def post(i):
            s, n = TILES[i]
            u_ref = ubs[i % 2]
            top = jnp.full((L_BLOCK, CTOK), -jnp.inf, F32)
            for r in range(0, n, L_BLOCK):
                u = u_ref[r:r + L_BLOCK, :]
                if s + r + L_BLOCK > MASK_FROM:
                    u = jnp.where(iota < limit - (s + r), u, -jnp.inf)
                    u_ref[r:r + L_BLOCK, :] = u
                top = jnp.maximum(top, u)
            m = jnp.max(top, axis=0, keepdims=True)
            if s + L_BLOCK > MASK_FROM:
                m = jnp.maximum(m, LOWEST)
            s8 = jnp.zeros((L_BLOCK, CTOK), F32)
            for r in range(0, n, L_BLOCK):
                u = u_ref[r:r + L_BLOCK, :]
                e = jnp.exp2((u - m) * EXP_SCALE)
                eb[s + r:s + r + L_BLOCK, :] = e
                s8 = s8 + e
                state[0] = state[0] + jnp.where(iota == (y - (s + r)), u, 0.0)
                if r % 64 == 64 - L_BLOCK:
                    yield 1
            tmax[slot, i:i + 1, :] = m
            tsum[slot, i:i + 1, :] = jnp.sum(s8, axis=0, keepdims=True)
            yield 1

        for _ in mm(lo):
            pass
        for i in range(lo + 1, hi):
            if before is not None and i in before:
                before[i]()
            interleave(mm(i), post(i - 1), 6)
        for _ in post(hi - 1):
            pass
        return state[0]

    def stat_copy(c, k):
        return pltpu.make_async_remote_copy(
            src_ref=stx.at[c], dst_ref=srx.at[c, k], send_sem=st_send.at[c, k], recv_sem=st_recv.at[c, k],
            device_id=(lax.rem(me + k, N_DEV),), device_id_type=MESH)

    def send_stats(c, tg):
        slot = lax.rem(c, 2)
        tm = tmax[slot]
        m_loc = jnp.max(tm, axis=0, keepdims=True)
        s_loc = jnp.sum(tsum[slot] * jnp.exp2((tm - m_loc) * EXP_SCALE), axis=0, keepdims=True)
        stx[c, 0:1, :] = m_loc
        stx[c, 1:2, :] = s_loc
        stx[c, 2:3, :] = jnp.sum(tg, axis=0, keepdims=True)
        for k in range(1, N_DEV):
            stat_copy(c, k).start()

    def recv_stats(c):
        slot = lax.rem(c, 2)
        for k in range(1, N_DEV):
            stat_copy(c, k).wait()
        parts = [stx[c]] + [srx[c, k] for k in range(1, N_DEV)]
        m_all = functools.reduce(jnp.maximum, [p[0:1] for p in parts])
        s_all = functools.reduce(jnp.add, [p[1:2] * jnp.exp2((p[0:1] - m_all) * EXP_SCALE) for p in parts])
        t_all = functools.reduce(jnp.add, [p[2:3] for p in parts])
        mask = mrow[c]
        weight = mask / mask_total
        lossv[...] += mask * (m_all / LOGIT_SCALE + jnp.log(s_all) - t_all / LOGIT_SCALE)
        crow[...] = jnp.exp2((tmax[slot] - m_all) * EXP_SCALE) * (weight / s_all)
        return weight

    def dz_out(c):
        return pltpu.make_async_copy(dzb.at[lax.rem(c, 2)], dz_hbm.at[:, pl.ds(pl.multiple_of(c * CTOK, CTOK), CTOK)], dz_sem.at[lax.rem(c, 2)])

    def dz_rows(c, weight, k):
        slot = lax.rem(c, 2)
        iota = lax.broadcasted_iota(jnp.int32, (DZ_BLOCK, CTOK), 0)
        y = yrow[c]
        s0, n0 = KTILES[k]
        for i, (s, n) in enumerate(TILES):
            if s0 <= s < s0 + n0:
                ci = crow[i:i + 1, :]
                for r in range(s, s + n, DZ_BLOCK):
                    e = ebuf[slot, r:r + DZ_BLOCK, :]
                    dzb[slot, r:r + DZ_BLOCK, :] = (e * ci - jnp.where(iota == (y - r), weight, 0.0)).astype(BF16)

    def dh_mm(c, k, half):
        s, n = KTILES[k]
        cols = slice(half * HALF, half * HALF + HALF)
        part = lax.dot_general(dzb[lax.rem(c, 2), s:s + n, :], emb[s:s + n, cols], (((0,), (0,)), ((), ())), preferred_element_type=F32)
        part = part.reshape(2, 2, 2, PIECE, HALF)
        if k == 0:
            acc[c, :, :, :, :, cols] = part
        else:
            acc[c, :, :, :, :, cols] += part

    def dg_part(c, half):
        cols = slice(half * HALF, half * HALF + HALF)
        total = jnp.zeros((8, HALF), F32)
        for r in range(CTOK // PIECE):
            inv = rcol[c, r][:, 0:1]
            xh = xv[c, r, :, cols].astype(F32) * inv
            total = total + fold8(acc[c, r // 4, (r // 2) % 2, r % 2, :, cols] * xh)
        dgv[:, cols] += jnp.sum(total, axis=0, keepdims=True)

    def rs_copy(c, half, stage):
        cols = pl.ds(half * HALF, HALF)
        if stage == 0:
            src, dst, dev = acc.at[c, :, :, 1 - core, :, cols], ra.at[c, half], peer_core
        elif stage == 1 and half == 0:
            src, dst, dev = acc.at[c, :, 1 - xc, core, :, cols], rb.at[c, half], peer_x
        elif stage == 1:
            src, dst, dev = acc.at[c, 1 - yc, :, core, :, cols], rb.at[c, half], peer_y
        elif half == 0:
            src, dst, dev = acc.at[c, 1 - yc, xc, core, :, cols], rc.at[c, half], peer_y
        else:
            src, dst, dev = acc.at[c, yc, 1 - xc, core, :, cols], rc.at[c, half], peer_x
        return pltpu.make_async_remote_copy(
            src_ref=src, dst_ref=dst, send_sem=rs_send.at[c, half, stage], recv_sem=rs_recv.at[c, half, stage],
            device_id=(dev,), device_id_type=MESH)

    def rs_start(c, half, stage):
        rs_copy(c, half, stage).start()

    def rs_finish(c, half, stage):
        rs_copy(c, half, stage).wait()
        cols = pl.ds(half * HALF, HALF)
        if stage == 0:
            acc[c, :, :, core, :, cols] += ra[c, half]
        elif stage == 1 and half == 0:
            acc[c, :, xc, core, :, cols] += rb[c, half]
        elif stage == 1:
            acc[c, yc, :, core, :, cols] += rb[c, half]
        else:
            acc[c, yc, xc, core, :, cols] += rc[c, half]
        if stage < 2:
            rs_start(c, half, stage + 1)

    def pair_finish(c, half):
        rs_copy(c, half, 0).wait()
        cols = slice(half * HALF, half * HALF + HALF)
        late = pl.ds(pl.multiple_of((c - EARLY) * PIECE, PIECE), PIECE)
        mine = pl.ds(pl.multiple_of(c * PIECE, PIECE), PIECE)

        def pair_sum(y, x):
            return acc[c, y, x, core, :, cols] + ra[c, half, y, x]

        own_out[mine, cols] = pair_sum(yc, xc)
        sx_out[late, cols] = pair_sum(yc, 1 - xc)
        sy_out[late, cols] = pair_sum(1 - yc, xc)
        sd_out[late, cols] = pair_sum(1 - yc, 1 - xc)

    def step(s, _):
        lc = jnp.minimum(s, CHUNKS - 1)
        dc = s - 1
        pc = jnp.maximum(s - 2, 0)

        @pl.when(s < CHUNKS)
        def _():
            send_stats(lc, logits(lc, 0, N_TILES, jnp.zeros((L_BLOCK, CTOK), F32)))

        @pl.when(s == 2)
        def _():
            rs_finish(0, 1, 0)

        @pl.when(s == 3)
        def _():
            rs_finish(0, 1, 1)
            rs_finish(1, 1, 0)
            rs_finish(0, 0, 2)

        @pl.when(s >= 3)
        def _():
            dz_out(dc).wait()

        weight = recv_stats(dc)
        dz_rows(dc, weight, 0)
        for k in range(1, len(KTILES)):
            dz_rows(dc, weight, k)
            dh_mm(dc, k - 1, 0)
        dh_mm(dc, len(KTILES) - 1, 0)
        dz_out(dc).start()
        rs_start(dc, 0, 0)

        @pl.when(jnp.logical_and(s >= 2, s < CHUNKS))
        def _():
            rs_finish(pc, 0, 1)

        @pl.when(s == CHUNKS)
        def _():
            pair_finish(CHUNKS - 2, 1)
            rs_finish(1, 1, 1)

        nc = jnp.minimum(s + 1, CHUNKS - 1)
        for k in range(len(KTILES)):
            dh_mm(dc, k, 1)
            if k == 1:
                dg_part(dc, 0)
            if k >= 2:
                norm_rows(nc, 2 * k - 4)
                norm_rows(nc, 2 * k - 3)
        ht[nc] = hs[nc].T
        rs_start(dc, 1, 0)
        dg_part(dc, 1)

        @pl.when(dc < EARLY)
        def _():
            rs_finish(dc, 0, 0)

        @pl.when(dc >= EARLY)
        def _():
            pair_finish(dc, 0)

        @pl.when(s == 3)
        def _():
            rs_finish(0, 1, 2)

        @pl.when(s == CHUNKS)
        def _():
            rs_finish(1, 0, 2)
        return 0

    x_copies[0].wait()
    norm_chunk(0)
    e_copies[0].wait()

    def more_rows(j):
        def run():
            e_copies[j].wait()
        return run

    tg0 = logits(0, 0, N_TILES, jnp.zeros((L_BLOCK, CTOK), F32), {E_SPLIT[j]: more_rows(j) for j in range(1, len(E_SPLIT))})
    pl.semaphore_wait(barrier, N_DEV - 1)
    send_stats(0, tg0)
    for c in range(1, CHUNKS):
        x_copies[c].wait()
    norm_chunk(1)
    lax.fori_loop(1, CHUNKS + 1, step, 0)
    h_copy = pltpu.make_async_copy(hs, h_hbm, h_sem)
    h_copy.start()

    dgsend[...] = dgv[...]
    dg_copy = pltpu.make_async_remote_copy(
        src_ref=dgsend, dst_ref=dgrx, send_sem=dg_send, recv_sem=dg_recv, device_id=(peer_core,), device_id_type=MESH)
    dg_copy.start()
    loss_out[...] = jnp.broadcast_to(jnp.sum(lossv[...], axis=1, keepdims=True) / mask_total, loss_out.shape)
    rs_finish(1, 1, 2)
    for c in range(EARLY):
        own_out[c * PIECE:(c + 1) * PIECE, :] = acc[c, yc, xc, core]
    pair_finish(CHUNKS - 1, 1)
    dg_copy.wait()
    dg_pair = dgv[...] + dgrx[...]
    dg_out[...] = dg_pair
    for out in (sx_out, sy_out, sd_out):
        out[LATE_ROWS:LATE_ROWS + 8, :] = jnp.broadcast_to(dg_pair, (8, DIM))
    h_copy.wait()
    dz_out(CHUNKS - 2).wait()
    dz_out(CHUNKS - 1).wait()


def norm_grad_kernel(own, rx, ry, rd, dg_pair, g_in, x_hbm, dx_out, dg_out, x, sem):
    copy = pltpu.make_async_copy(x_hbm.at[lax.axis_index("vp")], x, sem)
    copy.start()
    dg_out[...] = (dg_pair[...] + rx[LATE_ROWS:LATE_ROWS + 1, :] + ry[LATE_ROWS:LATE_ROWS + 1, :] + rd[LATE_ROWS:LATE_ROWS + 1, :]) / LOGIT_SCALE
    copy.wait()
    for c in range(CHUNKS):
        rows = slice(c * PIECE, (c + 1) * PIECE)
        dh = own[rows, :]
        if c >= EARLY:
            late = slice((c - EARLY) * PIECE, (c - EARLY + 1) * PIECE)
            dh = dh + rx[late, :] + ry[late, :] + rd[late, :]
        xf = x[rows, :].astype(F32)
        inv = lax.rsqrt(jnp.mean(xf * xf, axis=1, keepdims=True) + NORM_EPS)
        xh = xf * inv
        u = dh / LOGIT_SCALE * g_in[...]
        dx_out[rows, :] = inv * (u - xh * jnp.mean(u * xh, axis=1, keepdims=True))


D_FIRST, D_STEP, D_RING = 256, 768, 3
D_LOOPS = (ROWS - D_FIRST) // D_STEP
D_REST = ROWS - D_FIRST - D_LOOPS * D_STEP


def table_grad_kernel(dz_hbm, h_hbm, de_hbm, dz, h, ring, in_sem, h_sem, out_sem):
    tail = D_LOOPS + 1
    tail_row = ROWS - D_REST

    def fetch(i, row, rows):
        return pltpu.make_async_copy(dz_hbm.at[pl.ds(row, rows)], dz.at[pl.ds(row, rows)], in_sem.at[i])

    def store(slot, row, rows):
        return pltpu.make_async_copy(ring.at[slot, pl.ds(0, rows)], de_hbm.at[pl.ds(row, rows)], out_sem.at[slot])

    def row_of(i):
        return pl.multiple_of(D_FIRST + (i - 1) * D_STEP, 16)

    def tile(slot, row, rows):
        ring[slot, 0:rows, :] = jnp.dot(dz[pl.ds(row, rows), :], h[...], preferred_element_type=F32) * (1.0 / LOGIT_SCALE)
        store(slot, row, rows).start()

    h_copy = pltpu.make_async_copy(h_hbm, h, h_sem)
    fetch(0, 0, D_FIRST).start()
    h_copy.start()
    for i in (1, 2):
        fetch(i, D_FIRST + (i - 1) * D_STEP, D_STEP).start()
    h_copy.wait()
    fetch(0, 0, D_FIRST).wait()
    tile(0, 0, D_FIRST)

    def body(i, _):
        slot = lax.rem(i, D_RING)
        fetch(i, row_of(i), D_STEP).wait()

        @pl.when(i + 2 <= D_LOOPS)
        def _():
            fetch(i + 2, row_of(i + 2), D_STEP).start()

        @pl.when(i == D_LOOPS - 1)
        def _():
            fetch(tail, tail_row, D_REST).start()

        @pl.when(i == D_RING)
        def _():
            store(slot, 0, D_FIRST).wait()

        @pl.when(i > D_RING)
        def _():
            store(slot, 0, D_STEP).wait()

        tile(slot, row_of(i), D_STEP)
        return 0

    lax.fori_loop(1, D_LOOPS + 1, body, 0)
    fetch(tail, tail_row, D_REST).wait()
    store(tail % D_RING, 0, D_STEP).wait()
    tile(tail % D_RING, tail_row, D_REST)
    for i in range(tail - D_RING + 1, tail):
        store(i % D_RING, 0, D_STEP).wait()
    store(tail % D_RING, 0, D_REST).wait()


def solution(mesh):
    vp_axis = mesh.axis_names[0]
    vmem = pl.BlockSpec(memory_space=pltpu.VMEM)
    anywhere = pl.BlockSpec(memory_space=pl.ANY)
    dma = pltpu.SemaphoreType.DMA

    def local_step(residual, labels, loss_mask, norm_gain, table_shard):
        max_tile = max(n for _, n in TILES)
        dz, h, own, sx, sy, sd, dg_pair, loss = pl.pallas_call(
            main_kernel,
            out_shape=(
                jax.ShapeDtypeStruct((ROWS, TOKENS), BF16),
                jax.ShapeDtypeStruct((CHUNKS, CTOK, DIM), BF16),
                jax.ShapeDtypeStruct((TOKENS // N_DEV, DIM), F32),
                *[jax.ShapeDtypeStruct((LATE_ROWS + 8, DIM), F32)] * 3,
                jax.ShapeDtypeStruct((1, DIM), F32),
                jax.ShapeDtypeStruct((1, 128), F32),
            ),
            in_specs=[anywhere, vmem, vmem, vmem, anywhere],
            out_specs=(anywhere, anywhere, vmem, vmem, vmem, vmem, vmem, vmem),
            scratch_shapes=[
                pltpu.VMEM((ROWS, DIM), BF16),
                pltpu.VMEM((CHUNKS, N_DEV, PIECE, DIM), BF16),
                pltpu.VMEM((CHUNKS, CTOK, DIM), BF16),
                pltpu.VMEM((CHUNKS, DIM, CTOK), BF16),
                pltpu.VMEM((CHUNKS, N_DEV, PIECE, 128), F32),
                pltpu.VMEM((2, ROWS, CTOK), F32),
                pltpu.VMEM((2, ROWS, CTOK), BF16),
                pltpu.VMEM((CHUNKS, 2, 2, 2, PIECE, DIM), F32),
                pltpu.VMEM((max_tile, CTOK), F32),
                pltpu.VMEM((max_tile, CTOK), F32),
                pltpu.VMEM((CHUNKS, 1, CTOK), jnp.int32),
                pltpu.VMEM((CHUNKS, 1, CTOK), F32),
                pltpu.VMEM((2, N_TILES, CTOK), F32),
                pltpu.VMEM((2, N_TILES, CTOK), F32),
                pltpu.VMEM((N_TILES, CTOK), F32),
                pltpu.VMEM((CHUNKS, 8, CTOK), F32),
                pltpu.VMEM((CHUNKS, N_DEV, 8, CTOK), F32),
                pltpu.VMEM((1, CTOK), F32),
                pltpu.VMEM((1, DIM), F32),
                pltpu.VMEM((1, DIM), F32),
                pltpu.VMEM((1, DIM), F32),
                pltpu.VMEM((CHUNKS, 2, 2, 2, PIECE, HALF), F32),
                pltpu.VMEM((EARLY, 2, 2, PIECE, HALF), F32),
                pltpu.VMEM((EARLY, 2, PIECE, HALF), F32),
                dma((CHUNKS + len(E_SPLIT),)),
                dma,
                dma((2,)),
                dma((CHUNKS, N_DEV)),
                dma((CHUNKS, N_DEV)),
                dma((CHUNKS, 2, 3)),
                dma((CHUNKS, 2, 3)),
                dma,
                dma,
            ],
            compiler_params=pltpu.CompilerParams(collective_id=0, has_side_effects=True, vmem_limit_bytes=60 << 20),
            cost_estimate=pl.CostEstimate(flops=4 * ROWS * TOKENS * DIM, bytes_accessed=30 << 20, transcendentals=ROWS * TOKENS),
        )(
            residual.reshape(N_DEV, CHUNKS, PIECE, DIM),
            labels.reshape(N_DEV, 128),
            loss_mask.reshape(N_DEV, 128),
            norm_gain.reshape(1, DIM),
            table_shard,
        )
        rx, ry, rd = (lax.ppermute(v, vp_axis, [(i, i ^ k) for i in range(N_DEV)]) for v, k in ((sx, 2), (sy, 4), (sd, 6)))
        d_embed = pl.pallas_call(
            table_grad_kernel,
            out_shape=jax.ShapeDtypeStruct((ROWS, DIM), F32),
            in_specs=[anywhere, anywhere],
            out_specs=anywhere,
            scratch_shapes=[
                pltpu.VMEM((ROWS, TOKENS), BF16),
                pltpu.VMEM((TOKENS, DIM), BF16),
                pltpu.VMEM((D_RING, D_STEP, DIM), F32),
                dma((D_LOOPS + 2,)),
                dma,
                dma((D_RING,)),
            ],
            compiler_params=pltpu.CompilerParams(vmem_limit_bytes=60 << 20),
            cost_estimate=pl.CostEstimate(flops=2 * ROWS * TOKENS * DIM, bytes_accessed=40 << 20, transcendentals=0),
        )(dz, h.reshape(TOKENS, DIM))
        own_rows = TOKENS // N_DEV
        dx, dg = pl.pallas_call(
            norm_grad_kernel,
            out_shape=(jax.ShapeDtypeStruct((own_rows, DIM), F32), jax.ShapeDtypeStruct((1, DIM), F32)),
            in_specs=[vmem] * 6 + [anywhere],
            out_specs=(vmem, vmem),
            scratch_shapes=[pltpu.VMEM((own_rows, DIM), BF16), dma],
            compiler_params=pltpu.CompilerParams(vmem_limit_bytes=6 << 20),
            cost_estimate=pl.CostEstimate(flops=20 * own_rows * DIM, bytes_accessed=2 << 20, transcendentals=own_rows),
        )(own, rx, ry, rd, dg_pair, norm_gain.reshape(1, DIM), residual.reshape(N_DEV, own_rows, DIM))
        return loss[0, 0], dx, d_embed, dg[0]

    return jax.shard_map(local_step, mesh=mesh, in_specs=(P(), P(), P(), P(), P(vp_axis, None)), out_specs=(P(), P(vp_axis, None), P(vp_axis, None), P()), check_vma=False)
```

```python
import functools

import jax
import jax.numpy as jnp
from jax import lax
from jax.experimental import pallas as pl
from jax.experimental.pallas import tpu as pltpu
from jax.sharding import PartitionSpec as P

VOCAB_REAL = 49155
LOGIT_SCALE = 6.0
NORM_EPS = 1e-6
LOG2E = 1.4426950408889634
F32 = jnp.float32
BF16 = jnp.bfloat16
MESH = pl.DeviceIdType.MESH

N_DEV = 8
TOKENS = 1024
DIM = 1024
ROWS = 6176
CHUNKS = 4
CTOK = 256
PIECE = 32
HALF = DIM // 2
L_TILE = 128
K_TILE = 1024
DZ_BLOCK = 32
L_BLOCK = 16
LOWEST = float(jnp.finfo(jnp.float32).min)
MASK_FROM = VOCAB_REAL - (N_DEV - 1) * ROWS
EXP_SCALE = LOG2E / LOGIT_SCALE


def split_rows(step):
    cuts = [[i * step, step] for i in range(ROWS // step)]
    cuts[-1][1] = ROWS - cuts[-1][0]
    return [tuple(c) for c in cuts]


TILES = [(i * L_TILE, L_TILE) for i in range(ROWS // L_TILE)] + [(ROWS // L_TILE * L_TILE, ROWS % L_TILE)]
KTILES = split_rows(K_TILE)
N_TILES = len(TILES)
E_SPLIT = (0, 4, 10, 20, 32)
EARLY = 2
LATE_ROWS = (CHUNKS - EARLY) * PIECE


def fold8(v):
    return jnp.sum(v.reshape(v.shape[0] // 8, 8, v.shape[1]), axis=0)


def interleave(main, side, ratio):
    main_done = side_done = False
    while not (main_done and side_done):
        if not main_done:
            main_done = next(main, 0) == 0
        for _ in range(ratio):
            if not side_done:
                side_done = next(side, 0) == 0


def main_kernel(x_hbm, y_in, m_in, g_in, e_hbm,
                dz_hbm, h_hbm, own_out, sx_out, sy_out, sd_out, dg_out, loss_out,
                emb, xv, hs, ht, rcol, ebuf, dzb, acc, ub0, ub1, yrow, mrow,
                tmax, tsum, crow, stx, srx, lossv, dgv, dgsend, dgrx, ra, rb, rc,
                in_sem, h_sem, dz_sem, st_send, st_recv, rs_send, rs_recv, dg_send, dg_recv):
    me = lax.axis_index("vp")
    core = lax.rem(me, 2)
    xc = lax.rem(me // 2, 2)
    yc = me // 4
    peer_core = me + 1 - 2 * core
    peer_x = me + 2 - 4 * xc
    peer_y = me + 4 - 8 * yc

    e_cuts = [TILES[t][0] for t in E_SPLIT] + [ROWS]
    e_copies = [
        pltpu.make_async_copy(e_hbm.at[pl.ds(a, b - a)], emb.at[pl.ds(a, b - a)], in_sem.at[CHUNKS + j])
        for j, (a, b) in enumerate(zip(e_cuts[:-1], e_cuts[1:]))
    ]
    x_copies = [pltpu.make_async_copy(x_hbm.at[:, c], xv.at[c], in_sem.at[c]) for c in range(CHUNKS)]
    x_copies[0].start()
    for copy in e_copies:
        copy.start()
    for c in range(1, CHUNKS):
        x_copies[c].start()

    barrier = pltpu.get_barrier_semaphore()
    for k in range(1, N_DEV):
        pl.semaphore_signal(barrier, inc=1, device_id=(lax.rem(me + k, N_DEV),), device_id_type=MESH)

    lane = lax.broadcasted_iota(jnp.int32, (1, 128), 1) // PIECE
    base = me * ROWS
    for c in range(CHUNKS):
        for half in range(2):
            yh = jnp.zeros((1, 128), jnp.int32)
            mh = jnp.zeros((1, 128), F32)
            for i in range(4):
                row = half * 4 + i
                shift = (PIECE * (i - c)) % 128
                yr, mr = y_in[row:row + 1, :], m_in[row:row + 1, :]
                if shift:
                    yr, mr = pltpu.roll(yr, shift, 1), pltpu.roll(mr, shift, 1)
                yh = jnp.where(lane == i, yr, yh)
                mh = jnp.where(lane == i, mr, mh)
            yrow[c, :, half * 128:half * 128 + 128] = yh - base
            mrow[c, :, half * 128:half * 128 + 128] = mh
    mask_total = jnp.sum(jnp.sum(m_in[...], axis=0, keepdims=True), axis=1, keepdims=True)
    lossv[...] = jnp.zeros_like(lossv)
    dgv[...] = jnp.zeros_like(dgv)
    limit = VOCAB_REAL - base

    def norm_rows(c, r):
        xf = xv[c, r].astype(F32)
        inv = lax.rsqrt(jnp.mean(xf * xf, axis=1, keepdims=True) + NORM_EPS)
        rcol[c, r] = jnp.broadcast_to(inv, (PIECE, 128))
        hs[c, r * PIECE:(r + 1) * PIECE, :] = (xf * inv * g_in[...]).astype(BF16)

    def norm_chunk(c):
        for r in range(CTOK // PIECE):
            norm_rows(c, r)
        ht[c] = hs[c].T

    def logits(c, lo, hi, tg, before=None):
        slot = lax.rem(c, 2)
        iota = lax.broadcasted_iota(jnp.int32, (L_BLOCK, CTOK), 0)
        y = yrow[c]
        eb = ebuf.at[slot]
        ubs = (ub0, ub1)
        state = [tg]

        def mm(i):
            s, n = TILES[i]
            ubs[i % 2][0:n, :] = jnp.dot(emb[s:s + n, :], ht[c], preferred_element_type=F32)
            yield 1

        def post(i):
            s, n = TILES[i]
            u_ref = ubs[i % 2]
            top = jnp.full((L_BLOCK, CTOK), -jnp.inf, F32)
            for r in range(0, n, L_BLOCK):
                u = u_ref[r:r + L_BLOCK, :]
                if s + r + L_BLOCK > MASK_FROM:
                    u = jnp.where(iota < limit - (s + r), u, -jnp.inf)
                    u_ref[r:r + L_BLOCK, :] = u
                top = jnp.maximum(top, u)
            m = jnp.max(top, axis=0, keepdims=True)
            if s + L_BLOCK > MASK_FROM:
                m = jnp.maximum(m, LOWEST)
            s8 = jnp.zeros((L_BLOCK, CTOK), F32)
            for r in range(0, n, L_BLOCK):
                u = u_ref[r:r + L_BLOCK, :]
                e = jnp.exp2((u - m) * EXP_SCALE)
                eb[s + r:s + r + L_BLOCK, :] = e
                s8 = s8 + e
                state[0] = state[0] + jnp.where(iota == (y - (s + r)), u, 0.0)
                if r % 64 == 64 - L_BLOCK:
                    yield 1
            tmax[slot, i:i + 1, :] = m
            tsum[slot, i:i + 1, :] = jnp.sum(s8, axis=0, keepdims=True)
            yield 1

        for _ in mm(lo):
            pass
        for i in range(lo + 1, hi):
            if before is not None and i in before:
                before[i]()
            interleave(mm(i), post(i - 1), 6)
        for _ in post(hi - 1):
            pass
        return state[0]

    def stat_copy(c, k):
        return pltpu.make_async_remote_copy(
            src_ref=stx.at[c], dst_ref=srx.at[c, k], send_sem=st_send.at[c, k], recv_sem=st_recv.at[c, k],
            device_id=(lax.rem(me + k, N_DEV),), device_id_type=MESH)

    def send_stats(c, tg):
        slot = lax.rem(c, 2)
        tm = tmax[slot]
        m_loc = jnp.max(tm, axis=0, keepdims=True)
        s_loc = jnp.sum(tsum[slot] * jnp.exp2((tm - m_loc) * EXP_SCALE), axis=0, keepdims=True)
        stx[c, 0:1, :] = m_loc
        stx[c, 1:2, :] = s_loc
        stx[c, 2:3, :] = jnp.sum(tg, axis=0, keepdims=True)
        for k in range(1, N_DEV):
            stat_copy(c, k).start()

    def recv_stats(c):
        slot = lax.rem(c, 2)
        for k in range(1, N_DEV):
            stat_copy(c, k).wait()
        parts = [stx[c]] + [srx[c, k] for k in range(1, N_DEV)]
        m_all = functools.reduce(jnp.maximum, [p[0:1] for p in parts])
        s_all = functools.reduce(jnp.add, [p[1:2] * jnp.exp2((p[0:1] - m_all) * EXP_SCALE) for p in parts])
        t_all = functools.reduce(jnp.add, [p[2:3] for p in parts])
        mask = mrow[c]
        weight = mask / mask_total
        lossv[...] += mask * (m_all / LOGIT_SCALE + jnp.log(s_all) - t_all / LOGIT_SCALE)
        crow[...] = jnp.exp2((tmax[slot] - m_all) * EXP_SCALE) * (weight / s_all)
        return weight

    def dz_out(c):
        return pltpu.make_async_copy(dzb.at[lax.rem(c, 2)], dz_hbm.at[:, pl.ds(pl.multiple_of(c * CTOK, CTOK), CTOK)], dz_sem.at[lax.rem(c, 2)])

    def dz_rows(c, weight, k):
        slot = lax.rem(c, 2)
        iota = lax.broadcasted_iota(jnp.int32, (DZ_BLOCK, CTOK), 0)
        y = yrow[c]
        s0, n0 = KTILES[k]
        for i, (s, n) in enumerate(TILES):
            if s0 <= s < s0 + n0:
                ci = crow[i:i + 1, :]
                for r in range(s, s + n, DZ_BLOCK):
                    e = ebuf[slot, r:r + DZ_BLOCK, :]
                    dzb[slot, r:r + DZ_BLOCK, :] = (e * ci - jnp.where(iota == (y - r), weight, 0.0)).astype(BF16)

    def dh_mm(c, k, half):
        s, n = KTILES[k]
        cols = slice(half * HALF, half * HALF + HALF)
        part = lax.dot_general(dzb[lax.rem(c, 2), s:s + n, :], emb[s:s + n, cols], (((0,), (0,)), ((), ())), preferred_element_type=F32)
        part = part.reshape(2, 2, 2, PIECE, HALF)
        if k == 0:
            acc[c, :, :, :, :, cols] = part
        else:
            acc[c, :, :, :, :, cols] += part

    def dg_part(c, half):
        cols = slice(half * HALF, half * HALF + HALF)
        total = jnp.zeros((8, HALF), F32)
        for r in range(CTOK // PIECE):
            inv = rcol[c, r][:, 0:1]
            xh = xv[c, r, :, cols].astype(F32) * inv
            total = total + fold8(acc[c, r // 4, (r // 2) % 2, r % 2, :, cols] * xh)
        dgv[:, cols] += jnp.sum(total, axis=0, keepdims=True)

    def rs_copy(c, half, stage):
        cols = pl.ds(half * HALF, HALF)
        if stage == 0:
            src, dst, dev = acc.at[c, :, :, 1 - core, :, cols], ra.at[c, half], peer_core
        elif stage == 1 and half == 0:
            src, dst, dev = acc.at[c, :, 1 - xc, core, :, cols], rb.at[c, half], peer_x
        elif stage == 1:
            src, dst, dev = acc.at[c, 1 - yc, :, core, :, cols], rb.at[c, half], peer_y
        elif half == 0:
            src, dst, dev = acc.at[c, 1 - yc, xc, core, :, cols], rc.at[c, half], peer_y
        else:
            src, dst, dev = acc.at[c, yc, 1 - xc, core, :, cols], rc.at[c, half], peer_x
        return pltpu.make_async_remote_copy(
            src_ref=src, dst_ref=dst, send_sem=rs_send.at[c, half, stage], recv_sem=rs_recv.at[c, half, stage],
            device_id=(dev,), device_id_type=MESH)

    def rs_start(c, half, stage):
        rs_copy(c, half, stage).start()

    def rs_finish(c, half, stage):
        rs_copy(c, half, stage).wait()
        cols = pl.ds(half * HALF, HALF)
        if stage == 0:
            acc[c, :, :, core, :, cols] += ra[c, half]
        elif stage == 1 and half == 0:
            acc[c, :, xc, core, :, cols] += rb[c, half]
        elif stage == 1:
            acc[c, yc, :, core, :, cols] += rb[c, half]
        else:
            acc[c, yc, xc, core, :, cols] += rc[c, half]
        if stage < 2:
            rs_start(c, half, stage + 1)

    def pair_finish(c, half):
        rs_copy(c, half, 0).wait()
        cols = slice(half * HALF, half * HALF + HALF)
        late = pl.ds(pl.multiple_of((c - EARLY) * PIECE, PIECE), PIECE)
        mine = pl.ds(pl.multiple_of(c * PIECE, PIECE), PIECE)

        def pair_sum(y, x):
            return acc[c, y, x, core, :, cols] + ra[c, half, y, x]

        own_out[mine, cols] = pair_sum(yc, xc)
        sx_out[late, cols] = pair_sum(yc, 1 - xc)
        sy_out[late, cols] = pair_sum(1 - yc, xc)
        sd_out[late, cols] = pair_sum(1 - yc, 1 - xc)

    def step(s, _):
        lc = jnp.minimum(s, CHUNKS - 1)
        dc = s - 1
        pc = jnp.maximum(s - 2, 0)

        @pl.when(s < CHUNKS)
        def _():
            send_stats(lc, logits(lc, 0, N_TILES, jnp.zeros((L_BLOCK, CTOK), F32)))

        @pl.when(s == 2)
        def _():
            rs_finish(0, 1, 0)

        @pl.when(s == 3)
        def _():
            rs_finish(0, 1, 1)
            rs_finish(1, 1, 0)
            rs_finish(0, 0, 2)

        @pl.when(s >= 3)
        def _():
            dz_out(dc).wait()

        weight = recv_stats(dc)
        dz_rows(dc, weight, 0)
        for k in range(1, len(KTILES)):
            dz_rows(dc, weight, k)
            dh_mm(dc, k - 1, 0)
        dh_mm(dc, len(KTILES) - 1, 0)
        dz_out(dc).start()
        rs_start(dc, 0, 0)

        @pl.when(jnp.logical_and(s >= 2, s < CHUNKS))
        def _():
            rs_finish(pc, 0, 1)

        @pl.when(s == CHUNKS)
        def _():
            pair_finish(CHUNKS - 2, 1)
            rs_finish(1, 1, 1)

        nc = jnp.minimum(s + 1, CHUNKS - 1)
        for k in range(len(KTILES)):
            dh_mm(dc, k, 1)
            if k == 1:
                dg_part(dc, 0)
            if k >= 2:
                norm_rows(nc, 2 * k - 4)
                norm_rows(nc, 2 * k - 3)
        ht[nc] = hs[nc].T
        rs_start(dc, 1, 0)
        dg_part(dc, 1)

        @pl.when(dc < EARLY)
        def _():
            rs_finish(dc, 0, 0)

        @pl.when(dc >= EARLY)
        def _():
            pair_finish(dc, 0)

        @pl.when(s == 3)
        def _():
            rs_finish(0, 1, 2)

        @pl.when(s == CHUNKS)
        def _():
            rs_finish(1, 0, 2)
        return 0

    x_copies[0].wait()
    norm_chunk(0)
    e_copies[0].wait()

    def more_rows(j):
        def run():
            e_copies[j].wait()
        return run

    tg0 = logits(0, 0, N_TILES, jnp.zeros((L_BLOCK, CTOK), F32), {E_SPLIT[j]: more_rows(j) for j in range(1, len(E_SPLIT))})
    pl.semaphore_wait(barrier, N_DEV - 1)
    send_stats(0, tg0)
    for c in range(1, CHUNKS):
        x_copies[c].wait()
    norm_chunk(1)
    lax.fori_loop(1, CHUNKS + 1, step, 0)
    h_copy = pltpu.make_async_copy(hs, h_hbm, h_sem)
    h_copy.start()

    dgsend[...] = dgv[...]
    dg_copy = pltpu.make_async_remote_copy(
        src_ref=dgsend, dst_ref=dgrx, send_sem=dg_send, recv_sem=dg_recv, device_id=(peer_core,), device_id_type=MESH)
    dg_copy.start()
    loss_out[...] = jnp.broadcast_to(jnp.sum(lossv[...], axis=1, keepdims=True) / mask_total, loss_out.shape)
    rs_finish(1, 1, 2)
    for c in range(EARLY):
        own_out[c * PIECE:(c + 1) * PIECE, :] = acc[c, yc, xc, core]
    pair_finish(CHUNKS - 1, 1)
    dg_copy.wait()
    dg_pair = dgv[...] + dgrx[...]
    dg_out[...] = dg_pair
    for out in (sx_out, sy_out, sd_out):
        out[LATE_ROWS:LATE_ROWS + 8, :] = jnp.broadcast_to(dg_pair, (8, DIM))
    h_copy.wait()
    dz_out(CHUNKS - 2).wait()
    dz_out(CHUNKS - 1).wait()


def norm_grad_kernel(own, rx, ry, rd, dg_pair, g_in, x_hbm, dx_out, dg_out, x, sem):
    copy = pltpu.make_async_copy(x_hbm.at[lax.axis_index("vp")], x, sem)
    copy.start()
    dg_out[...] = (dg_pair[...] + rx[LATE_ROWS:LATE_ROWS + 1, :] + ry[LATE_ROWS:LATE_ROWS + 1, :] + rd[LATE_ROWS:LATE_ROWS + 1, :]) / LOGIT_SCALE
    copy.wait()
    for c in range(CHUNKS):
        rows = slice(c * PIECE, (c + 1) * PIECE)
        dh = own[rows, :]
        if c >= EARLY:
            late = slice((c - EARLY) * PIECE, (c - EARLY + 1) * PIECE)
            dh = dh + rx[late, :] + ry[late, :] + rd[late, :]
        xf = x[rows, :].astype(F32)
        inv = lax.rsqrt(jnp.mean(xf * xf, axis=1, keepdims=True) + NORM_EPS)
        xh = xf * inv
        u = dh / LOGIT_SCALE * g_in[...]
        dx_out[rows, :] = inv * (u - xh * jnp.mean(u * xh, axis=1, keepdims=True))


D_FIRST, D_STEP, D_RING = 256, 768, 3
D_LOOPS = (ROWS - D_FIRST) // D_STEP
D_REST = ROWS - D_FIRST - D_LOOPS * D_STEP


def table_grad_kernel(dz_hbm, h_hbm, de_hbm, dz, h, ring, in_sem, h_sem, out_sem):
    tail = D_LOOPS + 1
    tail_row = ROWS - D_REST

    def fetch(i, row, rows):
        return pltpu.make_async_copy(dz_hbm.at[pl.ds(row, rows)], dz.at[pl.ds(row, rows)], in_sem.at[i])

    def store(slot, row, rows):
        return pltpu.make_async_copy(ring.at[slot, pl.ds(0, rows)], de_hbm.at[pl.ds(row, rows)], out_sem.at[slot])

    def row_of(i):
        return pl.multiple_of(D_FIRST + (i - 1) * D_STEP, 16)

    def tile(slot, row, rows):
        ring[slot, 0:rows, :] = jnp.dot(dz[pl.ds(row, rows), :], h[...], preferred_element_type=F32) * (1.0 / LOGIT_SCALE)
        store(slot, row, rows).start()

    h_copy = pltpu.make_async_copy(h_hbm, h, h_sem)
    fetch(0, 0, D_FIRST).start()
    h_copy.start()
    for i in (1, 2):
        fetch(i, D_FIRST + (i - 1) * D_STEP, D_STEP).start()
    h_copy.wait()
    fetch(0, 0, D_FIRST).wait()
    tile(0, 0, D_FIRST)

    def body(i, _):
        slot = lax.rem(i, D_RING)
        fetch(i, row_of(i), D_STEP).wait()

        @pl.when(i + 2 <= D_LOOPS)
        def _():
            fetch(i + 2, row_of(i + 2), D_STEP).start()

        @pl.when(i == D_LOOPS - 1)
        def _():
            fetch(tail, tail_row, D_REST).start()

        @pl.when(i == D_RING)
        def _():
            store(slot, 0, D_FIRST).wait()

        @pl.when(i > D_RING)
        def _():
            store(slot, 0, D_STEP).wait()

        tile(slot, row_of(i), D_STEP)
        return 0

    lax.fori_loop(1, D_LOOPS + 1, body, 0)
    fetch(tail, tail_row, D_REST).wait()
    store(tail % D_RING, 0, D_STEP).wait()
    tile(tail % D_RING, tail_row, D_REST)
    for i in range(tail - D_RING + 1, tail):
        store(i % D_RING, 0, D_STEP).wait()
    store(tail % D_RING, 0, D_REST).wait()


def solution(mesh):
    vp_axis = mesh.axis_names[0]
    vmem = pl.BlockSpec(memory_space=pltpu.VMEM)
    anywhere = pl.BlockSpec(memory_space=pl.ANY)
    dma = pltpu.SemaphoreType.DMA

    def local_step(residual, labels, loss_mask, norm_gain, table_shard):
        max_tile = max(n for _, n in TILES)
        dz, h, own, sx, sy, sd, dg_pair, loss = pl.pallas_call(
            main_kernel,
            out_shape=(
                jax.ShapeDtypeStruct((ROWS, TOKENS), BF16),
                jax.ShapeDtypeStruct((CHUNKS, CTOK, DIM), BF16),
                jax.ShapeDtypeStruct((TOKENS // N_DEV, DIM), F32),
                *[jax.ShapeDtypeStruct((LATE_ROWS + 8, DIM), F32)] * 3,
                jax.ShapeDtypeStruct((1, DIM), F32),
                jax.ShapeDtypeStruct((1, 128), F32),
            ),
            in_specs=[anywhere, vmem, vmem, vmem, anywhere],
            out_specs=(anywhere, anywhere, vmem, vmem, vmem, vmem, vmem, vmem),
            scratch_shapes=[
                pltpu.VMEM((ROWS, DIM), BF16),
                pltpu.VMEM((CHUNKS, N_DEV, PIECE, DIM), BF16),
                pltpu.VMEM((CHUNKS, CTOK, DIM), BF16),
                pltpu.VMEM((CHUNKS, DIM, CTOK), BF16),
                pltpu.VMEM((CHUNKS, N_DEV, PIECE, 128), F32),
                pltpu.VMEM((2, ROWS, CTOK), F32),
                pltpu.VMEM((2, ROWS, CTOK), BF16),
                pltpu.VMEM((CHUNKS, 2, 2, 2, PIECE, DIM), F32),
                pltpu.VMEM((max_tile, CTOK), F32),
                pltpu.VMEM((max_tile, CTOK), F32),
                pltpu.VMEM((CHUNKS, 1, CTOK), jnp.int32),
                pltpu.VMEM((CHUNKS, 1, CTOK), F32),
                pltpu.VMEM((2, N_TILES, CTOK), F32),
                pltpu.VMEM((2, N_TILES, CTOK), F32),
                pltpu.VMEM((N_TILES, CTOK), F32),
                pltpu.VMEM((CHUNKS, 8, CTOK), F32),
                pltpu.VMEM((CHUNKS, N_DEV, 8, CTOK), F32),
                pltpu.VMEM((1, CTOK), F32),
                pltpu.VMEM((1, DIM), F32),
                pltpu.VMEM((1, DIM), F32),
                pltpu.VMEM((1, DIM), F32),
                pltpu.VMEM((CHUNKS, 2, 2, 2, PIECE, HALF), F32),
                pltpu.VMEM((EARLY, 2, 2, PIECE, HALF), F32),
                pltpu.VMEM((EARLY, 2, PIECE, HALF), F32),
                dma((CHUNKS + len(E_SPLIT),)),
                dma,
                dma((2,)),
                dma((CHUNKS, N_DEV)),
                dma((CHUNKS, N_DEV)),
                dma((CHUNKS, 2, 3)),
                dma((CHUNKS, 2, 3)),
                dma,
                dma,
            ],
            compiler_params=pltpu.CompilerParams(collective_id=0, has_side_effects=True, vmem_limit_bytes=60 << 20),
            cost_estimate=pl.CostEstimate(flops=4 * ROWS * TOKENS * DIM, bytes_accessed=30 << 20, transcendentals=ROWS * TOKENS),
        )(
            residual.reshape(N_DEV, CHUNKS, PIECE, DIM),
            labels.reshape(N_DEV, 128),
            loss_mask.reshape(N_DEV, 128),
            norm_gain.reshape(1, DIM),
            table_shard,
        )
        rx, ry, rd = (lax.ppermute(v, vp_axis, [(i, i ^ k) for i in range(N_DEV)]) for v, k in ((sx, 2), (sy, 4), (sd, 6)))
        d_embed = pl.pallas_call(
            table_grad_kernel,
            out_shape=jax.ShapeDtypeStruct((ROWS, DIM), F32),
            in_specs=[anywhere, anywhere],
            out_specs=anywhere,
            scratch_shapes=[
                pltpu.VMEM((ROWS, TOKENS), BF16),
                pltpu.VMEM((TOKENS, DIM), BF16),
                pltpu.VMEM((D_RING, D_STEP, DIM), F32),
                dma((D_LOOPS + 2,)),
                dma,
                dma((D_RING,)),
            ],
            compiler_params=pltpu.CompilerParams(vmem_limit_bytes=60 << 20),
            cost_estimate=pl.CostEstimate(flops=2 * ROWS * TOKENS * DIM, bytes_accessed=40 << 20, transcendentals=0),
        )(dz, h.reshape(TOKENS, DIM))
        own_rows = TOKENS // N_DEV
        dx, dg = pl.pallas_call(
            norm_grad_kernel,
            out_shape=(jax.ShapeDtypeStruct((own_rows, DIM), F32), jax.ShapeDtypeStruct((1, DIM), F32)),
            in_specs=[vmem] * 6 + [anywhere],
            out_specs=(vmem, vmem),
            scratch_shapes=[pltpu.VMEM((own_rows, DIM), BF16), dma],
            compiler_params=pltpu.CompilerParams(vmem_limit_bytes=6 << 20),
            cost_estimate=pl.CostEstimate(flops=20 * own_rows * DIM, bytes_accessed=2 << 20, transcendentals=own_rows),
        )(own, rx, ry, rd, dg_pair, norm_gain.reshape(1, DIM), residual.reshape(N_DEV, own_rows, DIM))
        return loss[0, 0], dx, d_embed, dg[0]

    return jax.shard_map(local_step, mesh=mesh, in_specs=(P(), P(), P(), P(), P(vp_axis, None)), out_specs=(P(), P(vp_axis, None), P(vp_axis, None), P()), check_vma=False)
```
